128 devices in a mesh: lev: 4 (over y), col: 32 (over z, x, core).
Axes of the slice: x: 4, y: 4, z: 4, core: 2. Of those that a mesh axis runs over, the one named last changes fastest.
Arguments:
- control_field: float32 [96, 16, 768, 128], P('lev', None, 'col'), may hold values from -24 to 24
- decay_rate: float32 [96, 768, 128], P('lev', 'col'), may hold values from 0.5 to 0.999
- diffusivity: float32 [768, 128], P('col'), may hold values from 0.08 to 0.24
Outputs:
- localized: float32 [96, 16, 768, 128], P('lev', None, 'col')
The draws below stay inside these ranges and needn't reach their ends.
All inputs are finite; a program needn't handle non-finite values.
Results may differ from the reference program's by a relative error of at most 0.00002.
Values sent between devices are 32-bit elements; how exact they have to be, the bound alone decides.
No kernel may reach another device: no remote copies, remote signals or barrier semaphores. Data moves between devices by JAX's collectives and lax.ppermute only.
A program may use at most 64 MiB of HBM per device.

```python
import math
import jax
import jax.numpy as jnp
from jax import lax

MEMBERS = 16
LATITUDE_ROWS = 128
SMOOTH = 4
WINDOW_LEVELS = 96
WINDOW_LONGITUDES = 768


def draw_decay_rate(key, part):
    key_scale = jax.random.fold_in(key, 11)
    key_rough = jax.random.fold_in(key, 12)
    spike_key = jax.random.fold_in(key, 13)
    depth_key = jax.random.fold_in(key, 14)
    low_scale = 4.0
    high_scale = 4.0 * WINDOW_LEVELS
    column_scale = jnp.exp(jax.random.uniform(key_scale, (1, WINDOW_LONGITUDES, LATITUDE_ROWS), jnp.float32, jnp.log(low_scale), jnp.log(high_scale)))
    roughness = jax.random.uniform(key_rough, (WINDOW_LEVELS, WINDOW_LONGITUDES, LATITUDE_ROWS), jnp.float32, 0.5, 1.5)
    decay_rates = jnp.exp(-1.0 / (column_scale * roughness))
    spike_levels = jax.random.randint(spike_key, (3,), 0, WINDOW_LEVELS)
    level_numbers = jnp.arange(WINDOW_LEVELS, dtype=jnp.int32)
    spike_present = jnp.any(level_numbers[:, None] == spike_levels[None, :], axis=1)
    spike_depth = jax.random.uniform(depth_key, (1, WINDOW_LONGITUDES, LATITUDE_ROWS), jnp.float32, 0.5, 0.8)
    decay_rates = jnp.where(spike_present[:, None, None], decay_rates * spike_depth, decay_rates)
    return jnp.clip(decay_rates, 0.5, 0.999).astype(jnp.float32)


def block_scale(rng, extent, cuts, low, high):
    gain, own = 1.0, jax.random.fold_in(rng, 6)
    for axis_at, parts in cuts:
        draws = jnp.exp(jax.random.uniform(jax.random.fold_in(own, axis_at), (parts,), jnp.float32, low / len(cuts), high / len(cuts)))
        gain = gain * jnp.repeat(draws, extent[axis_at] // parts).reshape([-1 if axis == axis_at else 1 for axis in range(len(extent))])
    return gain


def scatter_about(rng, extent, spread, most, split=(), held_as=jnp.bfloat16):
    entries = jax.random.normal(rng, extent, jnp.float32) * spread
    if len(split) > 0:
        entries = block_scale(rng, extent, split, -0.22, 0.18) * entries
    return jnp.clip(entries, min=-most, max=most).astype(held_as)


def setup_inputs(seed: int = 0) -> dict:
    seeds = jax.random.split(jax.random.key(seed), 4)
    control_field = scatter_about(seeds[0], (WINDOW_LEVELS, MEMBERS, WINDOW_LONGITUDES, LATITUDE_ROWS), 4.0, 24.0, ((0, 4), (2, 32)), jnp.float32)
    decay_rate = draw_decay_rate(jax.random.fold_in(seeds[3], 71), 0)
    diffusivity = jnp.clip(jnp.exp(math.log(0.24) - 1.0986123 * jax.random.uniform(seeds[2], (WINDOW_LONGITUDES, LATITUDE_ROWS), jnp.float32) ** block_scale(seeds[2], (WINDOW_LONGITUDES, LATITUDE_ROWS), ((0, 32),), -0.2, 0.2)), 0.08, 0.24)
    return dict(control_field=control_field, decay_rate=decay_rate, diffusivity=diffusivity)


def recursion(decay_rates, field, backward):
    def advance(state, inputs):
        weight, values = inputs
        state = weight * state + (1.0 - weight) * values
        return state, state

    start = jnp.zeros(field.shape[1:], jnp.float32)
    unused, swept = lax.scan(advance, start, (decay_rates[:, None], field), reverse=backward)
    return swept


def lat_sum(field):
    padded = jnp.pad(field, ((0, 0), (0, 0), (0, 0), (1, 1)))
    return padded[..., 2:] + padded[..., :-2]


def lon_sum(field):
    padded = jnp.pad(field, ((0, 0), (0, 0), (1, 1), (0, 0)))
    return padded[:, :, 2:] + padded[:, :, :-2]


def reference(control_field, decay_rate, diffusivity):
    filtered = control_field
    for repeat in range(2):
        filtered = recursion(decay_rate, filtered, False)
        filtered = recursion(decay_rate, filtered, True)
    current = filtered
    for position in range(SMOOTH):
        current = current + diffusivity[None, None] * (lon_sum(current) + lat_sum(current) - 4.0 * current)
    return current
```

```python
import functools

import jax
import jax.numpy as jnp
from jax import lax
from jax.experimental import pallas as pl
from jax.experimental.pallas import tpu as pltpu
from jax.sharding import PartitionSpec as P

SMOOTH = 4
LEVELS = 24
MEMBERS = 16
LONS = 24
LATS = 128
BLOCKS = 4
RECORD = 72
STATES = 64
GROUP = 4
CHUNKS = ((0, 4, 6),)
HALO_ROWS = LEVELS * GROUP * MEMBERS
MESSAGE_ROWS = HALO_ROWS + 8
PLANE_LEVELS = 2
STEP_LEVELS = 4

ANY = pl.BlockSpec(memory_space=pl.ANY)
F32 = jnp.float32


def shape(*dims):
    return jax.ShapeDtypeStruct(dims, F32)


def row(ref, at):
    return ref[pl.ds(at, 8, stride=0), :]


def responses(rates, profiles, scratch):
    tiles = [slice(8 * tile, 8 * tile + 8) for tile in range(LONS // 8)]
    up, down = range(LEVELS), range(LEVELS - 1, -1, -1)

    def sweep(order, source, target):
        state = [None] * len(tiles)
        for level in order:
            for at, lons in enumerate(tiles):
                rate = rates[level, lons, :]
                if source is None:
                    state[at] = rate if state[at] is None else rate * state[at]
                else:
                    value = (1.0 - rate) * source[level, lons, :]
                    state[at] = value if state[at] is None else rate * state[at] + value
                target[level, lons, :] = state[at]
        return state

    through = sweep(up, None, scratch.at[0])
    sweep(down, None, profiles.at[3])
    q21 = sweep(down, scratch.at[0], profiles.at[2])
    q32 = sweep(up, profiles.at[3], scratch.at[1])
    q31 = sweep(up, profiles.at[2], scratch.at[0])
    q42 = sweep(down, scratch.at[1], profiles.at[1])
    q41 = sweep(down, scratch.at[0], profiles.at[0])
    return through, q21, q31, q32, q41, q42


def sweep_kernel(chunk, first, field, rate, *refs):
    base, step, groups = chunk
    count = GROUP * groups
    share = count // BLOCKS
    if first:
        local, pieces, profiles_out, refs = refs[0], refs[1:5], refs[5], refs[6:]
    else:
        local, pieces, refs = refs[0], refs[1:5], refs[5:]
        profiles_out = None
    xs, rates, swept, exits, profiles, scratch, in_sems, out_sems = refs
    here = lax.axis_index("lev")
    rate_copy = pltpu.make_async_copy(rate, rates, in_sems.at[3])
    rate_copy.start()
    needed = sorted({(base + step * g) // 8 for g in range(groups)})
    loads = []
    for tile in needed:
        lons = pl.ds(8 * tile, 8)
        loads.append(pltpu.make_async_copy(field.at[:, lons, :], xs.at[:, lons, :], in_sems.at[tile]))
        loads[-1].start()
    rate_copy.wait()
    coefficients = responses(rates, profiles, scratch)
    outs = []
    if profiles_out is not None:
        outs.append(pltpu.make_async_copy(profiles, profiles_out, out_sems.at[4]))
        outs[-1].start()
    for at in range(count):
        lon = base + step * (at // GROUP) + at % GROUP
        for which, tiles in enumerate(coefficients):
            record = at * RECORD + STATES + which
            exits[record : record + 1, :] = tiles[lon // 8][lon % 8 : lon % 8 + 1, :]
    for load in loads:
        load.wait()
    values = xs.reshape(LEVELS * MEMBERS * LONS, LATS)
    weights = rates.reshape(LEVELS * LONS, LATS)

    def run(group, carry):
        lon = base + step * group
        for number in range(4):
            order = range(LEVELS) if number % 2 == 0 else range(LEVELS - 1, -1, -1)
            state = {}
            for level in order:
                for j in range(GROUP):
                    weight = row(weights, level * LONS + lon + j)
                    rest = 1.0 - weight
                    for half in range(2):
                        if number == 0:
                            start = (level * MEMBERS + 8 * half) * LONS + lon + j
                            value = values[pl.ds(start, 8, stride=LONS), :]
                        else:
                            value = swept[level, group * GROUP + j, 8 * half : 8 * half + 8, :]
                        value = rest * value
                        if (j, half) in state:
                            value = weight * state[j, half] + value
                        state[j, half] = value
                        swept[level, group * GROUP + j, 8 * half : 8 * half + 8, :] = value
            for (j, half), value in state.items():
                record = (group * GROUP + j) * RECORD + 16 * number + 8 * half
                exits[pl.ds(record, 8), :] = value
        return carry

    lax.fori_loop(0, groups, run, 0)
    for shift in range(BLOCKS):
        target = lax.rem(here + shift, BLOCKS)
        rows = pl.ds(target * (share * RECORD), share * RECORD)
        outs.append(pltpu.make_async_copy(exits.at[rows, :], pieces[shift], out_sems.at[shift]))
        outs[-1].start()
    outs.append(pltpu.make_async_copy(swept, local, out_sems.at[5]))
    outs[-1].start()
    for out in outs:
        out.wait()


def sweep_call(chunk, first, field, rate):
    count = GROUP * chunk[2]
    share = count // BLOCKS
    outs = [shape(LEVELS, count, MEMBERS, LATS)] + [shape(share * RECORD, LATS)] * BLOCKS
    if first:
        outs.append(shape(4, LEVELS, LONS, LATS))
    return pl.pallas_call(
        functools.partial(sweep_kernel, chunk, first),
        out_shape=outs,
        in_specs=[ANY] * 2,
        out_specs=[ANY] * len(outs),
        scratch_shapes=[
            pltpu.VMEM((LEVELS * MEMBERS, LONS, LATS), F32),
            pltpu.VMEM((LEVELS, LONS, LATS), F32),
            pltpu.VMEM((LEVELS, count, MEMBERS, LATS), F32),
            pltpu.VMEM((count * RECORD, LATS), F32),
            pltpu.VMEM((4, LEVELS, LONS, LATS), F32),
            pltpu.VMEM((2, LEVELS, LONS, LATS), F32),
            pltpu.SemaphoreType.DMA((4,)),
            pltpu.SemaphoreType.DMA((6,)),
        ],
        name="sweeps",
    )(field, rate)


def solve_kernel(share, *refs):
    pieces, outs, (records, states, in_sems, out_sems) = refs[:4], refs[4:8], refs[8:]
    here = lax.axis_index("lev")
    copies = []
    for shift in range(BLOCKS):
        source = lax.rem(here - shift + BLOCKS, BLOCKS)
        rows = pl.ds(source * (share * RECORD), share * RECORD)
        copies.append(pltpu.make_async_copy(pieces[shift], records.at[rows, :], in_sems.at[shift]))
        copies[-1].start()
    for copy in copies:
        copy.wait()

    def run(lon, carry):
        def exit_of(block, number, half):
            at = (block * share + lon) * RECORD + 16 * number + 8 * half
            return records[pl.ds(at, 8), :]

        def response(block, which):
            return row(records, (block * share + lon) * RECORD + STATES + which)

        for half in range(2):
            zero = jnp.zeros((8, LATS), F32)
            f1, b1, f2, b2 = ([zero] * BLOCKS for _ in range(4))
            for d in range(BLOCKS - 1):
                f1[d + 1] = exit_of(d, 0, half) + response(d, 0) * f1[d]
            for d in range(BLOCKS - 1, 0, -1):
                b1[d - 1] = exit_of(d, 1, half) + response(d, 1) * f1[d] + response(d, 0) * b1[d]
            for d in range(BLOCKS - 1):
                f2[d + 1] = (
                    exit_of(d, 2, half)
                    + response(d, 2) * f1[d]
                    + response(d, 3) * b1[d]
                    + response(d, 0) * f2[d]
                )
            for d in range(BLOCKS - 1, 0, -1):
                b2[d - 1] = (
                    exit_of(d, 3, half)
                    + response(d, 4) * f1[d]
                    + response(d, 5) * b1[d]
                    + response(d, 1) * f2[d]
                    + response(d, 0) * b2[d]
                )
            for d in range(BLOCKS):
                for number, entering in enumerate((f1, b1, f2, b2)):
                    at = (d * share + lon) * STATES + 16 * number + 8 * half
                    states[pl.ds(at, 8), :] = entering[d]
        return carry

    lax.fori_loop(0, share, run, 0)
    copies = []
    for shift in range(BLOCKS):
        target = lax.rem(here + shift, BLOCKS)
        rows = pl.ds(target * (share * STATES), share * STATES)
        copies.append(pltpu.make_async_copy(states.at[rows, :], outs[shift], out_sems.at[shift]))
        copies[-1].start()
    for copy in copies:
        copy.wait()


def solve_call(share, pieces):
    return pl.pallas_call(
        functools.partial(solve_kernel, share),
        out_shape=[shape(share * STATES, LATS)] * BLOCKS,
        in_specs=[ANY] * BLOCKS,
        out_specs=[ANY] * BLOCKS,
        scratch_shapes=[
            pltpu.VMEM((BLOCKS * share * RECORD, LATS), F32),
            pltpu.VMEM((BLOCKS * share * STATES, LATS), F32),
            pltpu.SemaphoreType.DMA((4,)),
            pltpu.SemaphoreType.DMA((4,)),
        ],
        name="solve",
    )(*pieces)


def gather_states(share, pieces, states, sems):
    here = lax.axis_index("lev")
    copies = []
    for shift in range(BLOCKS):
        source = lax.rem(here - shift + BLOCKS, BLOCKS)
        rows = pl.ds(source * (share * STATES), share * STATES)
        copies.append(pltpu.make_async_copy(pieces[shift], states.at[rows, :], sems.at[shift]))
        copies[-1].start()
    return copies


def corrected(local, profiles, entering):
    return local + profiles[0] * entering[0] + profiles[1] * entering[1] + profiles[2] * entering[2] + profiles[3] * entering[3]


def edge_kernel(chunk, local, profiles, diffusivity, *refs):
    base, step, groups = chunk
    share = groups
    pieces, outs = refs[:4], refs[4:6]
    block, rows, states, kappa, packed, in_sems, state_sems, out_sems = refs[6:]
    loads = gather_states(share, pieces, states, state_sems)
    for side, group in enumerate((0, groups - 1)):
        loads.append(pltpu.make_async_copy(local.at[:, pl.ds(group * GROUP, GROUP)], block.at[:, pl.ds(side * GROUP, GROUP)], in_sems.at[side]))
        loads[-1].start()
    loads.append(pltpu.make_async_copy(profiles, rows, in_sems.at[2]))
    loads[-1].start()
    loads.append(pltpu.make_async_copy(diffusivity, kappa, in_sems.at[3]))
    loads[-1].start()
    for load in loads:
        load.wait()
    profile_rows = rows.reshape(4 * LEVELS * LONS, LATS)
    for side, group in enumerate((0, groups - 1)):
        lon = base + step * group
        packed[side, HALO_ROWS : HALO_ROWS + 8, :] = kappa[(lon // 8) * 8 : (lon // 8) * 8 + 8, :]
        for j in range(GROUP):
            entering = [
                [states[(group * GROUP + j) * STATES + 16 * n + 8 * half : (group * GROUP + j) * STATES + 16 * n + 8 * half + 8, :] for n in range(4)]
                for half in range(2)
            ]

            def run(level, carry):
                mine = [row(profile_rows, (n * LEVELS + level) * LONS + lon + j) for n in range(4)]
                for half in range(2):
                    value = corrected(block[level, side * GROUP + j, 8 * half : 8 * half + 8, :], mine, entering[half])
                    packed[side, pl.ds(level * (GROUP * MEMBERS) + j * MEMBERS + 8 * half, 8), :] = value
                return carry

            lax.fori_loop(0, LEVELS, run, 0, unroll=8)
    copies = []
    for side in range(2):
        copies.append(pltpu.make_async_copy(packed.at[side], outs[side], out_sems.at[side]))
        copies[-1].start()
    for copy in copies:
        copy.wait()


def edge_call(chunk, local, profiles, diffusivity, pieces):
    share = chunk[2]
    return pl.pallas_call(
        functools.partial(edge_kernel, chunk),
        out_shape=[shape(MESSAGE_ROWS, LATS)] * 2,
        in_specs=[ANY] * 7,
        out_specs=[ANY] * 2,
        scratch_shapes=[
            pltpu.VMEM((LEVELS, 2 * GROUP, MEMBERS, LATS), F32),
            pltpu.VMEM((4, LEVELS, LONS, LATS), F32),
            pltpu.VMEM((BLOCKS * share * STATES, LATS), F32),
            pltpu.VMEM((LONS, LATS), F32),
            pltpu.VMEM((2, MESSAGE_ROWS, LATS), F32),
            pltpu.SemaphoreType.DMA((4,)),
            pltpu.SemaphoreType.DMA((4,)),
            pltpu.SemaphoreType.DMA((2,)),
        ],
        name="edges",
    )(local, profiles, diffusivity, *pieces)


def diffuse_kernel(chunks, *refs):
    n = len(chunks)
    locals_, refs = refs[:n], refs[n:]
    profiles, low, high, low_k, high_k, own_k, refs = *refs[:6], refs[6:]
    pieces, refs = refs[: 4 * n], refs[4 * n :]
    out, refs = refs[0], refs[1:]
    states, kappa, center, buffers, sems = refs[:n], *refs[n:]
    wide = LONS + 2 * GROUP

    @pl.when(pl.program_id(0) == 0)
    def _():
        copies = []
        for at, chunk in enumerate(chunks):
            copies += gather_states(chunk[2], pieces[4 * at : 4 * at + 4], states[at], sems.at[at])
        kappa[0:GROUP, :] = low_k[GROUP : 2 * GROUP, :]
        kappa[GROUP : GROUP + LONS, :] = own_k[...]
        kappa[GROUP + LONS : wide, :] = high_k[0:GROUP, :]
        center[...] = 1.0 - 4.0 * kappa[...]
        for copy in copies:
            copy.wait()

    where = {}
    for at, (base, step, groups) in enumerate(chunks):
        for index in range(GROUP * groups):
            where[base + step * (index // GROUP) + index % GROUP] = (at, index)
    profile_rows = profiles.reshape(4 * STEP_LEVELS * LONS, LATS)
    out_rows = out.reshape(STEP_LEVELS * MEMBERS * LONS, LATS)
    planes = [(level, half) for level in range(PLANE_LEVELS) for half in range(2)]
    lane = lax.broadcasted_iota(jnp.int32, (8, LATS), 1)
    first, last = lane == 0, lane == LATS - 1

    def run(part, carry):
        top = part * PLANE_LEVELS
        for lon in range(wide):
            own = lon - GROUP
            if 0 <= own < LONS:
                at, index = where[own]
                entering = [
                    [states[at][index * STATES + 16 * n + 8 * half : index * STATES + 16 * n + 8 * half + 8, :] for n in range(4)]
                    for half in range(2)
                ]
                for level in range(PLANE_LEVELS):
                    mine = [row(profile_rows, (n * STEP_LEVELS + top + level) * LONS + own) for n in range(4)]
                    for half in range(2):
                        value = corrected(locals_[at][top + level, index, 8 * half : 8 * half + 8, :], mine, entering[half])
                        buffers[0, 2 * level + half, lon] = value
            else:
                side, j = (low, lon) if own < 0 else (high, own - LONS)
                for level in range(PLANE_LEVELS):
                    for half in range(2):
                        start = (top + level) * (GROUP * MEMBERS) + j * MEMBERS + 8 * half
                        buffers[0, 2 * level + half, lon] = side[pl.ds(start, 8), :]
        for step in range(SMOOTH):
            source, target = step % 2, (step + 1) % 2
            west = [buffers[source, p, step] for p in range(len(planes))]
            here = [buffers[source, p, step + 1] for p in range(len(planes))]
            for lon in range(step + 1, wide - step - 1):
                k, c = row(kappa, lon), row(center, lon)
                for p, (level, half) in enumerate(planes):
                    east = buffers[source, p, lon + 1]
                    south = jnp.where(first, 0.0, pltpu.roll(here[p], 1, 1))
                    north = jnp.where(last, 0.0, pltpu.roll(here[p], LATS - 1, 1))
                    value = c * here[p] + k * ((east + west[p]) + (south + north))
                    west[p], here[p] = here[p], east
                    if step < SMOOTH - 1:
                        buffers[target, p, lon] = value
                    else:
                        start = ((top + level) * MEMBERS + 8 * half) * LONS + lon - GROUP
                        out_rows[pl.ds(start, 8, stride=LONS), :] = value
        return carry

    lax.fori_loop(0, STEP_LEVELS // PLANE_LEVELS, run, 0)


def diffuse_call(chunks, locals_, profiles, low, high, diffusivity, pieces):
    n = len(chunks)
    wide = LONS + 2 * GROUP
    rows = STEP_LEVELS * GROUP * MEMBERS
    fixed = lambda i: (HALO_ROWS // 8, 0)
    in_specs = [pl.BlockSpec((STEP_LEVELS, GROUP * chunk[2], MEMBERS, LATS), lambda i: (i, 0, 0, 0)) for chunk in chunks]
    in_specs += [
        pl.BlockSpec((4, STEP_LEVELS, LONS, LATS), lambda i: (0, i, 0, 0)),
        pl.BlockSpec((rows, LATS), lambda i: (i, 0)),
        pl.BlockSpec((rows, LATS), lambda i: (i, 0)),
        pl.BlockSpec((8, LATS), fixed),
        pl.BlockSpec((8, LATS), fixed),
        pl.BlockSpec((LONS, LATS), lambda i: (0, 0)),
    ]
    in_specs += [ANY] * (4 * n)
    return pl.pallas_call(
        functools.partial(diffuse_kernel, chunks),
        grid=(LEVELS // STEP_LEVELS,),
        out_shape=shape(LEVELS * MEMBERS, LONS, LATS),
        in_specs=in_specs,
        out_specs=pl.BlockSpec((STEP_LEVELS * MEMBERS, LONS, LATS), lambda i: (i, 0, 0)),
        scratch_shapes=[pltpu.VMEM((GROUP * chunk[2] * STATES, LATS), F32) for chunk in chunks]
        + [
            pltpu.VMEM((wide, LATS), F32),
            pltpu.VMEM((wide, LATS), F32),
            pltpu.VMEM((2, 2 * PLANE_LEVELS, wide, 8, LATS), F32),
            pltpu.SemaphoreType.DMA((n, 4)),
        ],
        name="diffuse",
    )(*locals_, profiles, low, high, low, high, diffusivity, *pieces)


def shifted(pieces):
    moved = [pieces[0]]
    for shift in (1, 2, 3):
        moved.append(lax.ppermute(pieces[shift], "lev", [(i, (i + shift) % BLOCKS) for i in range(BLOCKS)]))
    return moved


def per_device(control_field, decay_rate, diffusivity):
    field = control_field.reshape(LEVELS * MEMBERS, LONS, LATS)
    locals_, states, profiles = [], [], None
    for at, chunk in enumerate(CHUNKS):
        local, *rest = sweep_call(chunk, at == 0, field, decay_rate)
        if at == 0:
            profiles = rest.pop()
        locals_.append(local)
        states.append(shifted(solve_call(chunk[2], shifted(rest))))
    to_low, to_high = edge_call(CHUNKS[0], locals_[0], profiles, diffusivity, states[0])
    count = lax.axis_size("col")
    forward = [(i, i + 1) for i in range(count - 1)]
    low = lax.ppermute(to_high, "col", forward)
    high = lax.ppermute(to_low, "col", [(b, a) for a, b in forward])
    out = diffuse_call(CHUNKS, locals_, profiles, low, high, diffusivity, sum(states, []))
    return out.reshape(control_field.shape)


def solution(mesh):
    in_specs = (P("lev", None, "col", None), P("lev", "col", None), P("col", None))
    out_specs = P("lev", None, "col", None)
    return jax.shard_map(
        per_device, mesh=mesh, in_specs=in_specs, out_specs=out_specs, check_vma=False
    )
```

```python
import functools

import jax
import jax.numpy as jnp
from jax import lax
from jax.experimental import pallas as pl
from jax.experimental.pallas import tpu as pltpu
from jax.sharding import PartitionSpec as P

SMOOTH = 4
LEVELS = 24
MEMBERS = 16
LONS = 24
LATS = 128
BLOCKS = 4
SHARE = LONS // BLOCKS
RECORD = 72
STATES = 64
GROUP = 4
GROUPS = LONS // GROUP
SLAB = 8
SLABS = LEVELS // SLAB
PAD = LATS + 16

ANY = pl.BlockSpec(memory_space=pl.ANY)
F32 = jnp.float32


def shape(*dims):
    return jax.ShapeDtypeStruct(dims, F32)


def row(ref, at):
    return ref[pl.ds(at, 8, stride=0), :]


def slot(lon):
    if lon < GROUP:
        return lon * SHARE
    if lon >= LONS - GROUP:
        return (lon - LONS + GROUP) * SHARE + 1
    return (lon - GROUP) // GROUP * SHARE + 2 + lon % GROUP


def start_all(copies):
    for copy in copies:
        copy.start()
    return copies


def wait_all(copies):
    for copy in copies:
        copy.wait()


def responses(rates, profiles, scratch):
    tiles = [slice(8 * tile, 8 * tile + 8) for tile in range(LONS // 8)]
    up, down = range(LEVELS), range(LEVELS - 1, -1, -1)

    def sweep(order, source, target):
        state = [None] * len(tiles)
        for level in order:
            for at, lons in enumerate(tiles):
                rate = rates[level, lons, :]
                if source is None:
                    state[at] = rate if state[at] is None else rate * state[at]
                else:
                    value = (1.0 - rate) * source[level, lons, :]
                    state[at] = value if state[at] is None else rate * state[at] + value
                target[level, lons, :] = state[at]
        return state

    through = sweep(up, None, scratch.at[0])
    sweep(down, None, profiles.at[3])
    q21 = sweep(down, scratch.at[0], profiles.at[2])
    q32 = sweep(up, profiles.at[3], scratch.at[1])
    q31 = sweep(up, profiles.at[2], scratch.at[0])
    q42 = sweep(down, scratch.at[1], profiles.at[1])
    q41 = sweep(down, scratch.at[0], profiles.at[0])
    return through, q21, q31, q32, q41, q42


def sweep_kernel(field, rate, diffusivity, local, p0, p1, p2, p3, profiles_out, to_low, to_high, *refs):
    xs, rates, kappa, swept, exits, profiles, scratch, packed, in_sems, out_sems, local_sems, halo_sems = refs
    here = lax.axis_index("lev")
    small = start_all(
        [
            pltpu.make_async_copy(rate, rates, in_sems.at[3]),
            pltpu.make_async_copy(diffusivity, kappa, in_sems.at[4]),
        ]
    )
    loads = []
    for tile in range(LONS // 8):
        lons = pl.ds(8 * tile, 8)
        loads.append(pltpu.make_async_copy(field.at[:, lons, :], xs.at[:, lons, :], in_sems.at[tile]))
    start_all(loads)
    wait_all(small)
    coefficients = responses(rates, profiles, scratch)
    outs = start_all([pltpu.make_async_copy(profiles, profiles_out, out_sems.at[4])])
    for lon in range(LONS):
        for which, tiles in enumerate(coefficients):
            record = slot(lon) * RECORD + STATES + which
            exits[record : record + 1, :] = tiles[lon // 8][lon % 8 : lon % 8 + 1, :]
    profile_rows = profiles.reshape(4 * LEVELS * LONS, LATS)
    for side, lon in enumerate((0, LONS - GROUP)):
        packed[side, pl.ds(4, GROUP, stride=8), :] = kappa[lon : lon + GROUP, :]
        for level in range(LEVELS):
            for n in range(4):
                start = (n * LEVELS + level) * LONS + lon
                packed[side, pl.ds(level * GROUP * 8 + n, GROUP, stride=8), :] = profile_rows[pl.ds(start, GROUP), :]
    values = xs.reshape(LEVELS * MEMBERS * LONS, LATS)
    weights = rates.reshape(LEVELS * LONS, LATS)

    def save(group):
        lons = pl.ds(group * GROUP, GROUP)
        return pltpu.make_async_copy(swept.at[:, lons], local.at[:, lons], local_sems.at[group])

    def run(group, carry):
        lon = GROUP * group
        for number in range(4):
            order = range(LEVELS) if number % 2 == 0 else range(LEVELS - 1, -1, -1)
            state = {}
            for level in order:
                for j in range(GROUP):
                    weight = row(weights, level * LONS + lon + j)
                    rest = 1.0 - weight
                    for half in range(2):
                        if number == 0:
                            start = (level * MEMBERS + 8 * half) * LONS + lon + j
                            value = values[pl.ds(start, 8, stride=LONS), :]
                        else:
                            value = swept[level, lon + j, 8 * half : 8 * half + 8, :]
                        value = rest * value
                        if (j, half) in state:
                            value = weight * state[j, half] + value
                        state[j, half] = value
                        swept[level, lon + j, 8 * half : 8 * half + 8, :] = value
            for (j, half), value in state.items():
                edge = jnp.where(group == 0, j * SHARE, j * SHARE + 1)
                inner = (group - 1) * SHARE + 2 + j
                place = jnp.where((group == 0) | (group == GROUPS - 1), edge, inner)
                exits[pl.ds(pl.multiple_of(place * RECORD + 16 * number + 8 * half, 8), 8), :] = value
        save(group).start()
        return carry

    for tile in range(LONS // 8):
        loads[tile].wait()
        lax.fori_loop(2 * tile, 2 * tile + 2, run, 0)
    for shift, piece in enumerate((p0, p1, p2, p3)):
        target = lax.rem(here + shift, BLOCKS)
        rows = pl.ds(target * (SHARE * RECORD), SHARE * RECORD)
        outs += start_all([pltpu.make_async_copy(exits.at[rows, :], piece, out_sems.at[shift])])
    for side, (lon, out) in enumerate(((0, to_low), (LONS - GROUP, to_high))):
        outs += start_all(
            [
                pltpu.make_async_copy(swept.at[:, pl.ds(lon, GROUP)], out.at[:, :, pl.ds(0, MEMBERS), :], halo_sems.at[2 * side]),
                pltpu.make_async_copy(
                    packed.at[side].reshape(LEVELS, GROUP, 8, LATS), out.at[:, :, pl.ds(MEMBERS, 8), :], halo_sems.at[2 * side + 1]
                ),
            ]
        )
    wait_all(outs)
    wait_all([save(group) for group in range(GROUPS)])


def sweep_call(field, rate, diffusivity):
    halo = shape(LEVELS, GROUP, MEMBERS + 8, LATS)
    outs = [shape(LEVELS, LONS, MEMBERS, LATS)] + [shape(SHARE * RECORD, LATS)] * BLOCKS
    outs += [shape(4, LEVELS, LONS, LATS), halo, halo]
    return pl.pallas_call(
        sweep_kernel,
        out_shape=outs,
        in_specs=[ANY] * 3,
        out_specs=[ANY] * len(outs),
        scratch_shapes=[
            pltpu.VMEM((LEVELS * MEMBERS, LONS, LATS), F32),
            pltpu.VMEM((LEVELS, LONS, LATS), F32),
            pltpu.VMEM((LONS, LATS), F32),
            pltpu.VMEM((LEVELS, LONS, MEMBERS, LATS), F32),
            pltpu.VMEM((LONS * RECORD, LATS), F32),
            pltpu.VMEM((4, LEVELS, LONS, LATS), F32),
            pltpu.VMEM((2, LEVELS, LONS, LATS), F32),
            pltpu.VMEM((2, LEVELS * GROUP * 8, LATS), F32),
            pltpu.SemaphoreType.DMA((5,)),
            pltpu.SemaphoreType.DMA((5,)),
            pltpu.SemaphoreType.DMA((GROUPS,)),
            pltpu.SemaphoreType.DMA((4,)),
        ],
        name="sweeps",
    )(field, rate, diffusivity)


def solve_kernel(*refs):
    pieces, outs, (records, states, in_sems, out_sems) = refs[:4], refs[4:8], refs[8:]
    here = lax.axis_index("lev")
    copies = []
    for shift in range(BLOCKS):
        source = lax.rem(here - shift + BLOCKS, BLOCKS)
        rows = pl.ds(source * (SHARE * RECORD), SHARE * RECORD)
        copies.append(pltpu.make_async_copy(pieces[shift], records.at[rows, :], in_sems.at[shift]))
    wait_all(start_all(copies))

    def run(lon, carry):
        def exit_of(block, number, half):
            at = (block * SHARE + lon) * RECORD + 16 * number + 8 * half
            return records[pl.ds(pl.multiple_of(at, 8), 8), :]

        def response(block, which):
            return row(records, (block * SHARE + lon) * RECORD + STATES + which)

        for half in range(2):
            zero = jnp.zeros((8, LATS), F32)
            f1, b1, f2, b2 = ([zero] * BLOCKS for _ in range(4))
            for d in range(BLOCKS - 1):
                f1[d + 1] = exit_of(d, 0, half) + response(d, 0) * f1[d]
            for d in range(BLOCKS - 1, 0, -1):
                b1[d - 1] = exit_of(d, 1, half) + response(d, 1) * f1[d] + response(d, 0) * b1[d]
            for d in range(BLOCKS - 1):
                f2[d + 1] = (
                    exit_of(d, 2, half)
                    + response(d, 2) * f1[d]
                    + response(d, 3) * b1[d]
                    + response(d, 0) * f2[d]
                )
            for d in range(BLOCKS - 1, 0, -1):
                b2[d - 1] = (
                    exit_of(d, 3, half)
                    + response(d, 4) * f1[d]
                    + response(d, 5) * b1[d]
                    + response(d, 1) * f2[d]
                    + response(d, 0) * b2[d]
                )
            for d in range(BLOCKS):
                for number, entering in enumerate((f1, b1, f2, b2)):
                    at = (d * SHARE + lon) * STATES + 16 * number + 8 * half
                    states[pl.ds(pl.multiple_of(at, 8), 8), :] = entering[d]
        return carry

    lax.fori_loop(0, SHARE, run, 0)
    copies = []
    for shift in range(BLOCKS):
        target = lax.rem(here + shift, BLOCKS)
        rows = pl.ds(target * (SHARE * STATES), SHARE * STATES)
        copies.append(pltpu.make_async_copy(states.at[rows, :], outs[shift], out_sems.at[shift]))
    wait_all(start_all(copies))


def solve_call(pieces):
    return pl.pallas_call(
        solve_kernel,
        out_shape=[shape(SHARE * STATES, LATS)] * BLOCKS,
        in_specs=[ANY] * BLOCKS,
        out_specs=[ANY] * BLOCKS,
        scratch_shapes=[
            pltpu.VMEM((BLOCKS * SHARE * RECORD, LATS), F32),
            pltpu.VMEM((BLOCKS * SHARE * STATES, LATS), F32),
            pltpu.SemaphoreType.DMA((4,)),
            pltpu.SemaphoreType.DMA((4,)),
        ],
        name="solve",
    )(*pieces)


def pieces_into(pieces, target, rows_each, sems):
    here = lax.axis_index("lev")
    copies = []
    for shift, piece in enumerate(pieces):
        source = lax.rem(here - shift + BLOCKS, BLOCKS)
        rows = pl.ds(pl.multiple_of(source * rows_each, 8), rows_each)
        copies.append(pltpu.make_async_copy(piece, target.at[rows, :], sems.at[shift]))
    return copies


def corrected_block(value_of, profile_of, entering):
    parts = []
    for level in range(SLAB):
        mine = [profile_of(n, level) for n in range(4)]
        for half in range(2):
            value = value_of(level, half)
            for n in range(4):
                value = value + mine[n] * entering[half][n]
            parts.append(value)
    return jnp.concatenate(parts, axis=0)


def entering_of(states, start):
    return [[states[start + 16 * n + 8 * half : start + 16 * n + 8 * half + 8, :] for n in range(4)] for half in range(2)]


def spread(kappa_row):
    return jnp.transpose(jnp.broadcast_to(kappa_row, (LATS, LATS)))


def diffuse(rows, spread_rows, base, wide):
    slots = rows.shape[0] // (2 * PAD)

    def at(which, lon, offset):
        return (which * slots + base + lon) * PAD + 8 + offset

    for step in range(SMOOTH):
        source, target = step % 2, (step + 1) % 2

        def tile(t, carry):
            top = pl.multiple_of(8 * t, 8)
            west = rows[pl.ds(at(source, step, top), 8), :]
            here = rows[pl.ds(at(source, step + 1, top), 8), :]
            for lon in range(step + 1, wide - step - 1):
                east = rows[pl.ds(at(source, lon + 1, top), 8), :]
                north = rows[pl.ds(at(source, lon, top - 1), 8), :]
                south = rows[pl.ds(at(source, lon, top + 1), 8), :]
                k = spread_rows[base + lon, pl.ds(top, 8), :]
                around = (east + west) + (north + south)
                rows[pl.ds(at(target, lon, top), 8), :] = here + k * (around - 4.0 * here)
                west, here = here, east
            return carry

        lax.fori_loop(0, LATS // 8, tile, 0, unroll=2)


def clear_pads(buffers):
    zero = jnp.zeros((8, LATS), F32)
    for which in range(2):
        for lon in range(buffers.shape[1]):
            buffers[which, lon, 0:8, :] = zero
            buffers[which, lon, PAD - 8 : PAD, :] = zero


def inner_kernel(local, profiles, diffusivity, s0, s1, s2, s3, out, *refs):
    ls, rows, states, kappa, spread_rows, buffers, made, in_sems, state_sems, local_sems, out_sems = refs
    first = start_all(
        pieces_into((s0, s1, s2, s3), states, SHARE * STATES, state_sems)
        + [pltpu.make_async_copy(diffusivity, kappa, in_sems.at[0]), pltpu.make_async_copy(profiles, rows, in_sems.at[1])]
    )

    def load(slab):
        levels = pl.ds(slab * SLAB, SLAB)
        return pltpu.make_async_copy(local.at[levels], ls.at[levels], local_sems.at[slab])

    def save(slab):
        part = pl.ds(slab * SLAB * MEMBERS, SLAB * MEMBERS)
        return pltpu.make_async_copy(made.at[part], out.at[part], out_sems.at[slab])

    for slab in range(SLABS):
        load(slab).start()
    clear_pads(buffers)
    wait_all(first)
    for lon in range(LONS):
        spread_rows[lon] = spread(kappa[lon : lon + 1, :])
    profile_rows = rows.reshape(4 * LEVELS * LONS, LATS)
    made_rows = made.reshape(LEVELS * MEMBERS * LONS, LATS)
    flat = buffers.reshape(2 * LONS * PAD, LATS)

    def run(slab, carry):
        load(slab).wait()
        for lon in range(LONS):
            block = corrected_block(
                lambda level, half: ls[slab * SLAB + level, lon, 8 * half : 8 * half + 8, :],
                lambda n, level: row(profile_rows, (n * LEVELS + slab * SLAB + level) * LONS + lon),
                entering_of(states, slot(lon) * STATES),
            )
            buffers[0, lon, 8 : 8 + LATS, :] = jnp.transpose(block)
        diffuse(flat, spread_rows, 0, LONS)
        for lon in range(GROUP, LONS - GROUP):
            block = jnp.transpose(buffers[0, lon, 8 : 8 + LATS, :])
            for part in range(2 * SLAB):
                start = (slab * SLAB * MEMBERS + 8 * part) * LONS + lon
                made_rows[pl.ds(start, 8, stride=LONS), :] = block[8 * part : 8 * part + 8, :]
        save(slab).start()
        return carry

    lax.fori_loop(0, SLABS, run, 0)
    wait_all([save(slab) for slab in range(SLABS)])


def inner_call(local, profiles, diffusivity, pieces):
    return pl.pallas_call(
        inner_kernel,
        out_shape=shape(LEVELS * MEMBERS, LONS, LATS),
        in_specs=[ANY] * 7,
        out_specs=ANY,
        scratch_shapes=[
            pltpu.VMEM((LEVELS, LONS, MEMBERS, LATS), F32),
            pltpu.VMEM((4, LEVELS, LONS, LATS), F32),
            pltpu.VMEM((LONS * STATES, LATS), F32),
            pltpu.VMEM((LONS, LATS), F32),
            pltpu.VMEM((LONS, LATS, LATS), F32),
            pltpu.VMEM((2, LONS, PAD, LATS), F32),
            pltpu.VMEM((LEVELS * MEMBERS, LONS, LATS), F32),
            pltpu.SemaphoreType.DMA((2,)),
            pltpu.SemaphoreType.DMA((4,)),
            pltpu.SemaphoreType.DMA((SLABS,)),
            pltpu.SemaphoreType.DMA((SLABS,)),
        ],
        cost_estimate=pl.CostEstimate(flops=10**8, transcendentals=0, bytes_accessed=10**7),
        name="inner",
    )(local, profiles, diffusivity, *pieces)


def outer_kernel(begun, local, profiles, diffusivity, s0, s1, s2, s3, low, high, low_s, high_s, out, *refs):
    ls, rows, states, kappa, spread_rows, buffers, made, halos, halo_states, *sems = refs
    in_sems, state_sems, halo_sems, local_sems, begun_sems, out_sems = sems
    here = lax.axis_index("lev")
    first = start_all(
        pieces_into((s0, s1, s2, s3), states, SHARE * STATES, state_sems)
        + [pltpu.make_async_copy(diffusivity, kappa, in_sems.at[0]), pltpu.make_async_copy(profiles, rows, in_sems.at[1])]
        + [
            pltpu.make_async_copy(source.at[pl.ds(shift * STATES, STATES), :], halo_states.at[side, lax.rem(here - shift + BLOCKS, BLOCKS)], halo_sems.at[side, shift])
            for side, source in enumerate((low_s, high_s))
            for shift in range(BLOCKS)
        ]
    )

    def loads(slab):
        levels = pl.ds(slab * SLAB, SLAB)
        part = pl.ds(slab * SLAB * MEMBERS, SLAB * MEMBERS)
        copies = []
        for side, (halo, lon) in enumerate(((low, 0), (high, 16))):
            copies.append(pltpu.make_async_copy(local.at[levels, pl.ds(lon, 8)], ls.at[side, levels], local_sems.at[slab, side]))
            copies.append(pltpu.make_async_copy(halo.at[levels], halos.at[side, levels], local_sems.at[slab, 2 + side]))
            copies.append(pltpu.make_async_copy(begun.at[part, pl.ds(lon, 8), :], made.at[side, part], begun_sems.at[slab, side]))
        return copies

    def saves(slab):
        part = pl.ds(slab * SLAB * MEMBERS, SLAB * MEMBERS)
        return [
            pltpu.make_async_copy(made.at[side, part], out.at[part, pl.ds(lon, 8), :], out_sems.at[slab, side])
            for side, lon in enumerate((0, 16))
        ]

    for slab in range(SLABS):
        start_all(loads(slab))
    clear_pads(buffers)
    wait_all(first)
    wait_all(loads(0))
    for side in range(2):
        for j in range(8):
            lon = 16 * side + j
            at = 4 + j if side == 0 else 12 + j
            spread_rows[at] = spread(kappa[lon : lon + 1, :])
        for j in range(GROUP):
            spread_rows[j if side == 0 else 20 + j] = spread(halos[side, 0, j, MEMBERS + 4 : MEMBERS + 5, :])
    profile_rows = rows.reshape(4 * LEVELS * LONS, LATS)
    halo_rows = halos.reshape(2 * LEVELS * GROUP * (MEMBERS + 8), LATS)
    made_rows = made.reshape(2 * LEVELS * MEMBERS * 8, LATS)
    flat = buffers.reshape(2 * LONS * PAD, LATS)

    def run(slab, carry):
        @pl.when(slab > 0)
        def _():
            wait_all(loads(slab))

        for side in range(2):
            for j in range(8):
                lon = 16 * side + j
                at = 4 + j if side == 0 else 12 + j
                block = corrected_block(
                    lambda level, half: ls[side, slab * SLAB + level, j, 8 * half : 8 * half + 8, :],
                    lambda n, level: row(profile_rows, (n * LEVELS + slab * SLAB + level) * LONS + lon),
                    entering_of(states, slot(lon) * STATES),
                )
                buffers[0, at, 8 : 8 + LATS, :] = jnp.transpose(block)
            for j in range(GROUP):
                at = j if side == 0 else 20 + j
                block = corrected_block(
                    lambda level, half: halos[side, slab * SLAB + level, j, 8 * half : 8 * half + 8, :],
                    lambda n, level: row(halo_rows, ((side * LEVELS + slab * SLAB + level) * GROUP + j) * (MEMBERS + 8) + MEMBERS + n),
                    entering_of(halo_states.at[side, j], 0),
                )
                buffers[0, at, 8 : 8 + LATS, :] = jnp.transpose(block)
        for side in range(2):
            diffuse(flat, spread_rows, 12 * side, 12)
        for side in range(2):
            for j in range(GROUP):
                block = jnp.transpose(buffers[0, 12 * side + 4 + j, 8 : 8 + LATS, :])
                for part in range(2 * SLAB):
                    start = ((side * LEVELS + slab * SLAB) * MEMBERS + 8 * part) * 8 + 4 * side + j
                    made_rows[pl.ds(start, 8, stride=8), :] = block[8 * part : 8 * part + 8, :]
        start_all(saves(slab))
        return carry

    lax.fori_loop(0, SLABS, run, 0)
    for slab in range(SLABS):
        wait_all(saves(slab))


def outer_call(begun, local, profiles, diffusivity, pieces, low, high, low_s, high_s):
    return pl.pallas_call(
        outer_kernel,
        out_shape=shape(LEVELS * MEMBERS, LONS, LATS),
        in_specs=[ANY] * 12,
        out_specs=ANY,
        input_output_aliases={0: 0},
        scratch_shapes=[
            pltpu.VMEM((2, LEVELS, 8, MEMBERS, LATS), F32),
            pltpu.VMEM((4, LEVELS, LONS, LATS), F32),
            pltpu.VMEM((LONS * STATES, LATS), F32),
            pltpu.VMEM((LONS, LATS), F32),
            pltpu.VMEM((LONS, LATS, LATS), F32),
            pltpu.VMEM((2, LONS, PAD, LATS), F32),
            pltpu.VMEM((2, LEVELS * MEMBERS, 8, LATS), F32),
            pltpu.VMEM((2, LEVELS, GROUP, MEMBERS + 8, LATS), F32),
            pltpu.VMEM((2, GROUP, STATES, LATS), F32),
            pltpu.SemaphoreType.DMA((2,)),
            pltpu.SemaphoreType.DMA((4,)),
            pltpu.SemaphoreType.DMA((2, 4)),
            pltpu.SemaphoreType.DMA((SLABS, 4)),
            pltpu.SemaphoreType.DMA((SLABS, 2)),
            pltpu.SemaphoreType.DMA((SLABS, 2)),
        ],
        name="outer",
    )(begun, local, profiles, diffusivity, *pieces, low, high, low_s, high_s)


def shifted(pieces):
    moved = [pieces[0]]
    for shift in (1, 2, 3):
        moved.append(lax.ppermute(pieces[shift], "lev", [(i, (i + shift) % BLOCKS) for i in range(BLOCKS)]))
    return moved


def exchanged(to_low, to_high):
    count = lax.axis_size("col")
    forward = [(i, i + 1) for i in range(count - 1)]
    backward = [(b, a) for a, b in forward]
    return lax.ppermute(to_high, "col", forward), lax.ppermute(to_low, "col", backward)


def per_device(control_field, decay_rate, diffusivity):
    field = control_field.reshape(LEVELS * MEMBERS, LONS, LATS)
    local, *pieces, profiles, to_low, to_high = sweep_call(field, decay_rate, diffusivity)
    pieces = shifted(pieces)
    low, high = exchanged(to_low, to_high)
    states = shifted(solve_call(pieces))
    low_s, high_s = exchanged(
        jnp.concatenate([piece[:STATES] for piece in states]),
        jnp.concatenate([piece[STATES : 2 * STATES] for piece in states]),
    )
    begun = inner_call(local, profiles, diffusivity, states)
    out = outer_call(begun, local, profiles, diffusivity, states, low, high, low_s, high_s)
    return out.reshape(control_field.shape)


def solution(mesh):
    in_specs = (P("lev", None, "col", None), P("lev", "col", None), P("col", None))
    out_specs = P("lev", None, "col", None)
    return jax.shard_map(
        per_device, mesh=mesh, in_specs=in_specs, out_specs=out_specs, check_vma=False
    )
```

```python
import functools

import jax
import jax.numpy as jnp
from jax import lax
from jax.experimental import pallas as pl
from jax.experimental.pallas import tpu as pltpu
from jax.sharding import PartitionSpec as P

SMOOTH = 4
LEVELS = 24
MEMBERS = 16
LONS = 24
LATS = 128
BLOCKS = 4
SHARE = LONS // BLOCKS
RECORD = 72
STATES = 64
GROUP = 4
GROUPS = LONS // GROUP
SLAB = 8
SLABS = LEVELS // SLAB
PAD = LATS + 16

OFF_CHIP = pl.BlockSpec(memory_space=pltpu.HBM)
ON_CHIP = pl.BlockSpec(memory_space=pltpu.VMEM)
ROOM = pltpu.CompilerParams(vmem_limit_bytes=28 * 2**20)
F32 = jnp.float32


def shape(*dims):
    return jax.ShapeDtypeStruct(dims, F32)


def resident(*dims):
    return pltpu.VMEM(dims, F32)


def row(ref, at):
    return ref[pl.ds(at, 8, stride=0), :]


def slot(lon):
    if lon < GROUP:
        return lon * SHARE
    if lon >= LONS - GROUP:
        return (lon - LONS + GROUP) * SHARE + 1
    return (lon - GROUP) // GROUP * SHARE + 2 + lon % GROUP


def start_all(copies):
    for copy in copies:
        copy.start()
    return copies


def wait_all(copies):
    for copy in copies:
        copy.wait()


def in_order(pieces, target, rows):
    here = lax.axis_index("lev")
    for shift, piece in enumerate(pieces):
        source = lax.rem(here - shift + BLOCKS, BLOCKS)
        target[pl.ds(pl.multiple_of(source * rows, 8), rows), :] = piece[...]


def responses(rates, profiles, scratch):
    tiles = [slice(8 * tile, 8 * tile + 8) for tile in range(LONS // 8)]
    up, down = range(LEVELS), range(LEVELS - 1, -1, -1)

    def sweep(order, source, target):
        state = [None] * len(tiles)
        for level in order:
            for at, lons in enumerate(tiles):
                rate = rates[level, lons, :]
                if source is None:
                    state[at] = rate if state[at] is None else rate * state[at]
                else:
                    value = (1.0 - rate) * source[level, lons, :]
                    state[at] = value if state[at] is None else rate * state[at] + value
                target[level, lons, :] = state[at]
        return state

    through = sweep(up, None, scratch.at[0])
    sweep(down, None, profiles.at[3])
    q21 = sweep(down, scratch.at[0], profiles.at[2])
    q32 = sweep(up, profiles.at[3], scratch.at[1])
    q31 = sweep(up, profiles.at[2], scratch.at[0])
    q42 = sweep(down, scratch.at[1], profiles.at[1])
    q41 = sweep(down, scratch.at[0], profiles.at[0])
    return through, q21, q31, q32, q41, q42


def sweep_kernel(field, rate, diffusivity, local, p0, p1, p2, p3, profiles, to_low, to_high, xs, rates, kappa, exits, scratch, sems):
    here = lax.axis_index("lev")
    small = start_all([pltpu.make_async_copy(rate, rates, sems.at[3]), pltpu.make_async_copy(diffusivity, kappa, sems.at[4])])
    loads = []
    for tile in range(LONS // 8):
        lons = pl.ds(8 * tile, 8)
        loads.append(pltpu.make_async_copy(field.at[:, lons, :], xs.at[:, lons, :], sems.at[tile]))
    start_all(loads)
    wait_all(small)
    coefficients = responses(rates, profiles, scratch)
    for lon in range(LONS):
        for which, tiles in enumerate(coefficients):
            record = slot(lon) * RECORD + STATES + which
            exits[record : record + 1, :] = tiles[lon // 8][lon % 8 : lon % 8 + 1, :]
    profile_rows = profiles.reshape(4 * LEVELS * LONS, LATS)
    height = MEMBERS + 8
    for lon, out in ((0, to_low), (LONS - GROUP, to_high)):
        packed = out.reshape(LEVELS * GROUP * height, LATS)
        packed[pl.ds(MEMBERS + 4, GROUP, stride=height), :] = kappa[lon : lon + GROUP, :]
        for level in range(LEVELS):
            for n in range(4):
                start = (n * LEVELS + level) * LONS + lon
                packed[pl.ds(level * GROUP * height + MEMBERS + n, GROUP, stride=height), :] = profile_rows[pl.ds(start, GROUP), :]
    values = xs.reshape(LEVELS * MEMBERS * LONS, LATS)
    weights = rates.reshape(LEVELS * LONS, LATS)

    def run(group, carry):
        lon = GROUP * group
        for number in range(4):
            order = range(LEVELS) if number % 2 == 0 else range(LEVELS - 1, -1, -1)
            state = {}
            for level in order:
                for j in range(GROUP):
                    weight = row(weights, level * LONS + lon + j)
                    rest = 1.0 - weight
                    for half in range(2):
                        if number == 0:
                            start = (level * MEMBERS + 8 * half) * LONS + lon + j
                            value = values[pl.ds(start, 8, stride=LONS), :]
                        else:
                            value = local[level, lon + j, 8 * half : 8 * half + 8, :]
                        value = rest * value
                        if (j, half) in state:
                            value = weight * state[j, half] + value
                        state[j, half] = value
                        local[level, lon + j, 8 * half : 8 * half + 8, :] = value
            for (j, half), value in state.items():
                edge = jnp.where(group == 0, j * SHARE, j * SHARE + 1)
                inner = (group - 1) * SHARE + 2 + j
                place = jnp.where((group == 0) | (group == GROUPS - 1), edge, inner)
                exits[pl.ds(pl.multiple_of(place * RECORD + 16 * number + 8 * half, 8), 8), :] = value
        return carry

    for tile in range(LONS // 8):
        loads[tile].wait()
        lax.fori_loop(2 * tile, 2 * tile + 2, run, 0)
    for shift, piece in enumerate((p0, p1, p2, p3)):
        target = lax.rem(here + shift, BLOCKS)
        piece[...] = exits[pl.ds(pl.multiple_of(target * (SHARE * RECORD), 8), SHARE * RECORD), :]
    for lon, out in ((0, to_low), (LONS - GROUP, to_high)):
        for j in range(GROUP):
            out[:, j, 0:MEMBERS, :] = local[:, lon + j]


def sweep_call(field, rate, diffusivity):
    halo = resident(LEVELS, GROUP, MEMBERS + 8, LATS)
    outs = [resident(LEVELS, LONS, MEMBERS, LATS)] + [resident(SHARE * RECORD, LATS)] * BLOCKS
    outs += [resident(4, LEVELS, LONS, LATS), halo, halo]
    return pl.pallas_call(
        sweep_kernel,
        out_shape=outs,
        in_specs=[OFF_CHIP] * 3,
        out_specs=[ON_CHIP] * len(outs),
        scratch_shapes=[
            pltpu.VMEM((LEVELS * MEMBERS, LONS, LATS), F32),
            pltpu.VMEM((LEVELS, LONS, LATS), F32),
            pltpu.VMEM((LONS, LATS), F32),
            pltpu.VMEM((LONS * RECORD, LATS), F32),
            pltpu.VMEM((2, LEVELS, LONS, LATS), F32),
            pltpu.SemaphoreType.DMA((5,)),
        ],
        compiler_params=ROOM,
        name="sweeps",
    )(*(pltpu.with_memory_space_constraint(x, pltpu.HBM) for x in (field, rate, diffusivity)))


def solve_kernel(*refs):
    pieces, outs, (records, states) = refs[:4], refs[4:8], refs[8:]
    here = lax.axis_index("lev")
    in_order(pieces, records, SHARE * RECORD)

    def run(lon, carry):
        def exit_of(block, number, half):
            at = (block * SHARE + lon) * RECORD + 16 * number + 8 * half
            return records[pl.ds(pl.multiple_of(at, 8), 8), :]

        def response(block, which):
            return row(records, (block * SHARE + lon) * RECORD + STATES + which)

        for half in range(2):
            zero = jnp.zeros((8, LATS), F32)
            f1, b1, f2, b2 = ([zero] * BLOCKS for _ in range(4))
            for d in range(BLOCKS - 1):
                f1[d + 1] = exit_of(d, 0, half) + response(d, 0) * f1[d]
            for d in range(BLOCKS - 1, 0, -1):
                b1[d - 1] = exit_of(d, 1, half) + response(d, 1) * f1[d] + response(d, 0) * b1[d]
            for d in range(BLOCKS - 1):
                f2[d + 1] = (
                    exit_of(d, 2, half)
                    + response(d, 2) * f1[d]
                    + response(d, 3) * b1[d]
                    + response(d, 0) * f2[d]
                )
            for d in range(BLOCKS - 1, 0, -1):
                b2[d - 1] = (
                    exit_of(d, 3, half)
                    + response(d, 4) * f1[d]
                    + response(d, 5) * b1[d]
                    + response(d, 1) * f2[d]
                    + response(d, 0) * b2[d]
                )
            for d in range(BLOCKS):
                for number, entering in enumerate((f1, b1, f2, b2)):
                    at = (d * SHARE + lon) * STATES + 16 * number + 8 * half
                    states[pl.ds(pl.multiple_of(at, 8), 8), :] = entering[d]
        return carry

    lax.fori_loop(0, SHARE, run, 0)
    for shift, out in enumerate(outs):
        target = lax.rem(here + shift, BLOCKS)
        out[...] = states[pl.ds(pl.multiple_of(target * (SHARE * STATES), 8), SHARE * STATES), :]


def solve_call(pieces):
    return pl.pallas_call(
        solve_kernel,
        out_shape=[resident(SHARE * STATES, LATS)] * BLOCKS,
        in_specs=[ON_CHIP] * BLOCKS,
        out_specs=[ON_CHIP] * BLOCKS,
        scratch_shapes=[
            pltpu.VMEM((BLOCKS * SHARE * RECORD, LATS), F32),
            pltpu.VMEM((BLOCKS * SHARE * STATES, LATS), F32),
        ],
        compiler_params=ROOM,
        name="solve",
    )(*pieces)


def corrected_block(value_of, profile_of, entering):
    parts = []
    for level in range(SLAB):
        mine = [profile_of(n, level) for n in range(4)]
        for half in range(2):
            value = value_of(level, half)
            for n in range(4):
                value = value + mine[n] * entering[half][n]
            parts.append(value)
    return jnp.concatenate(parts, axis=0)


def entering_of(states, start):
    return [[states[start + 16 * n + 8 * half : start + 16 * n + 8 * half + 8, :] for n in range(4)] for half in range(2)]


def spread(kappa_row):
    return jnp.transpose(jnp.broadcast_to(kappa_row, (LATS, LATS)))


def stepped(here, around, k):
    return here + k * (around - 4.0 * here)


def clear_pads(rows, blocks):
    zero = jnp.zeros((8, LATS), F32)
    for block in range(blocks):
        rows[block * PAD : block * PAD + 8, :] = zero
        rows[block * PAD + LATS + 8 : (block + 1) * PAD, :] = zero


def inner_kernel(local, profiles, kappa, s0, s1, s2, s3, out, begun, kept, spread_rows, states, buffers, made, sems):
    def save(slab):
        part = pl.ds(slab * SLAB * MEMBERS, SLAB * MEMBERS)
        return pltpu.make_async_copy(made.at[part], out.at[part, pl.ds(8, 8), :], sems.at[slab])

    in_order((s0, s1, s2, s3), states, SHARE * STATES)
    rows = buffers.reshape(2 * LONS * PAD, LATS)
    kept_rows = kept.reshape(SLABS * 2 * 2 * SMOOTH * PAD, LATS)
    clear_pads(rows, 2 * LONS)
    clear_pads(kept_rows, SLABS * 2 * 2 * SMOOTH)
    for lon in range(LONS):
        spread_rows[lon] = spread(kappa[lon : lon + 1, :])
    profile_rows = profiles.reshape(4 * LEVELS * LONS, LATS)
    made_rows = made.reshape(LEVELS * MEMBERS * 8, LATS)
    begun_rows = begun.reshape(2 * LEVELS * MEMBERS * 8, LATS)

    def run(slab, carry):
        def keep(step, lon):
            for side, m in enumerate((lon, LONS - 1 - lon)):
                if step <= m < step + 2 and step < SMOOTH:
                    return ((slab * 2 + side) * 2 * SMOOTH + 2 * step + m - step) * PAD + 8
            return None

        for lon in range(LONS):
            block = jnp.transpose(
                corrected_block(
                    lambda level, half: local[slab * SLAB + level, lon, 8 * half : 8 * half + 8, :],
                    lambda n, level: row(profile_rows, (n * LEVELS + slab * SLAB + level) * LONS + lon),
                    entering_of(states, slot(lon) * STATES),
                )
            )
            buffers[0, lon, 8 : 8 + LATS, :] = block
            start = keep(0, lon)
            if start is not None:
                kept_rows[pl.ds(pl.multiple_of(start, 8), LATS), :] = block
        for step in range(SMOOTH):

            def at(which, lon, offset):
                return (which * LONS + lon) * PAD + 8 + offset

            def tile(t, carry):
                source, target = step % 2, (step + 1) % 2
                top = pl.multiple_of(8 * t, 8)
                west = rows[pl.ds(at(source, step, top), 8), :]
                here = rows[pl.ds(at(source, step + 1, top), 8), :]
                for lon in range(step + 1, LONS - step - 1):
                    east = rows[pl.ds(at(source, lon + 1, top), 8), :]
                    north = rows[pl.ds(at(source, lon, top - 1), 8), :]
                    south = rows[pl.ds(at(source, lon, top + 1), 8), :]
                    k = spread_rows[lon, pl.ds(top, 8), :]
                    value = stepped(here, (east + west) + (north + south), k)
                    rows[pl.ds(at(target, lon, top), 8), :] = value
                    start = keep(step + 1, lon)
                    if start is not None:
                        kept_rows[pl.ds(pl.multiple_of(start + top, 8), 8), :] = value
                    west, here = here, east
                return carry

            lax.fori_loop(0, LATS // 8, tile, 0, unroll=2)
        for lon in range(GROUP, LONS - GROUP):
            block = jnp.transpose(buffers[0, lon, 8 : 8 + LATS, :])
            for part in range(2 * SLAB):
                first = slab * SLAB * MEMBERS + 8 * part
                piece = block[8 * part : 8 * part + 8, :]
                if 8 <= lon < 16:
                    made_rows[pl.ds(first * 8 + lon - 8, 8, stride=8), :] = piece
                else:
                    side = lon // 16
                    begun_rows[pl.ds((side * LEVELS * MEMBERS + first) * 8 + lon - 16 * side, 8, stride=8), :] = piece
        save(slab).start()
        return carry

    lax.fori_loop(0, SLABS, run, 0)
    wait_all([save(slab) for slab in range(SLABS)])


def inner_call(local, profiles, diffusivity, pieces):
    return pl.pallas_call(
        inner_kernel,
        out_shape=[
            shape(LEVELS * MEMBERS, LONS, LATS),
            resident(2, LEVELS * MEMBERS, 8, LATS),
            resident(SLABS, 2, 2 * SMOOTH, PAD, LATS),
            resident(LONS, LATS, LATS),
        ],
        in_specs=[ON_CHIP] * 7,
        out_specs=[OFF_CHIP, ON_CHIP, ON_CHIP, ON_CHIP],
        scratch_shapes=[
            pltpu.VMEM((LONS * STATES, LATS), F32),
            pltpu.VMEM((2, LONS, PAD, LATS), F32),
            pltpu.VMEM((LEVELS * MEMBERS, 8, LATS), F32),
            pltpu.SemaphoreType.DMA((SLABS,)),
        ],
        compiler_params=ROOM,
        cost_estimate=pl.CostEstimate(flops=10**8, transcendentals=0, bytes_accessed=10**7),
        name="inner",
    )(local, profiles, diffusivity, *pieces)


def outer_kernel(whole, begun, kept, spread_rows, low, high, low_s, high_s, out, filled, buffers, halo_spread, sems):
    here = lax.axis_index("lev")
    places = 2 * SMOOTH

    def saves(slab):
        part = pl.ds(slab * SLAB * MEMBERS, SLAB * MEMBERS)
        return [
            pltpu.make_async_copy(filled.at[side, part], out.at[part, pl.ds(lon, 8), :], sems.at[slab, side])
            for side, lon in enumerate((0, 16))
        ]

    rows = buffers.reshape(2 * 2 * places * PAD, LATS)
    kept_rows = kept.reshape(SLABS * 2 * 2 * SMOOTH * PAD, LATS)
    clear_pads(rows, 2 * 2 * places)
    height = MEMBERS + 8
    halos = [(low, low_s), (high, high_s)]
    for side, (halo, _) in enumerate(halos):
        for j in range(GROUP):
            place = j if side == 0 else GROUP - 1 - j
            halo_spread[side, place] = spread(halo[0, j, MEMBERS + 4 : MEMBERS + 5, :])
    filled_rows = filled.reshape(2 * LEVELS * MEMBERS * 8, LATS)

    def run(slab, carry):
        for side, (halo, halo_states) in enumerate(halos):
            halo_rows = halo.reshape(LEVELS * GROUP * height, LATS)
            for j in range(GROUP):
                place = j if side == 0 else GROUP - 1 - j
                start = lax.rem(here - j + BLOCKS, BLOCKS) * STATES
                entering = [
                    [halo_states[pl.ds(pl.multiple_of(start + 16 * n + 8 * half, 8), 8), :] for n in range(4)] for half in range(2)
                ]
                block = corrected_block(
                    lambda level, half: halo[slab * SLAB + level, j, 8 * half : 8 * half + 8, :],
                    lambda n, level: row(halo_rows, ((slab * SLAB + level) * GROUP + j) * height + MEMBERS + n),
                    entering,
                )
                buffers[0, side, place, 8 : 8 + LATS, :] = jnp.transpose(block)
        for step in range(SMOOTH):

            def tile(t, carry):
                top = pl.multiple_of(8 * t, 8)
                for side in range(2):

                    def value_at(place, offset):
                        if place < step + SMOOTH:
                            start = ((step % 2 * 2 + side) * places + place) * PAD
                            return rows[pl.ds(start + 8 + top + offset, 8), :]
                        start = ((slab * 2 + side) * 2 * SMOOTH + 2 * step + place - step - SMOOTH) * PAD
                        return kept_rows[pl.ds(start + 8 + top + offset, 8), :]

                    west, here = value_at(step, 0), value_at(step + 1, 0)
                    for place in range(step + 1, step + SMOOTH + 1):
                        east = value_at(place + 1, 0)
                        around = (east + west) + (value_at(place, -1) + value_at(place, 1))
                        if place < GROUP:
                            k = halo_spread[side, place, pl.ds(top, 8), :]
                        else:
                            m = place - GROUP
                            k = spread_rows[m if side == 0 else LONS - 1 - m, pl.ds(top, 8), :]
                        start = (((step + 1) % 2 * 2 + side) * places + place) * PAD
                        rows[pl.ds(pl.multiple_of(start + 8 + top, 8), 8), :] = stepped(here, around, k)
                        west, here = here, east
                return carry

            lax.fori_loop(0, LATS // 8, tile, 0, unroll=2)
        for side in range(2):
            for m in range(GROUP):
                block = jnp.transpose(buffers[0, side, GROUP + m, 8 : 8 + LATS, :])
                for part in range(2 * SLAB):
                    first = (side * LEVELS + slab * SLAB) * MEMBERS + 8 * part
                    lon = m if side == 0 else 7 - m
                    filled_rows[pl.ds(first * 8 + lon, 8, stride=8), :] = block[8 * part : 8 * part + 8, :]
        start_all(saves(slab))
        return carry

    lax.fori_loop(0, SLABS, run, 0)
    for slab in range(SLABS):
        wait_all(saves(slab))


def outer_call(whole, begun, kept, spread_rows, low, high, low_s, high_s):
    return pl.pallas_call(
        outer_kernel,
        out_shape=[shape(LEVELS * MEMBERS, LONS, LATS), resident(2, LEVELS * MEMBERS, 8, LATS)],
        in_specs=[OFF_CHIP] + [ON_CHIP] * 7,
        out_specs=[OFF_CHIP, ON_CHIP],
        input_output_aliases={0: 0, 1: 1},
        scratch_shapes=[
            pltpu.VMEM((2, 2, 2 * SMOOTH, PAD, LATS), F32),
            pltpu.VMEM((2, GROUP, LATS, LATS), F32),
            pltpu.SemaphoreType.DMA((SLABS, 2)),
        ],
        compiler_params=ROOM,
        name="outer",
    )(whole, begun, kept, spread_rows, low, high, low_s, high_s)


def shifted(pieces):
    moved = [pieces[0]]
    for shift in (1, 2, 3):
        moved.append(lax.ppermute(pieces[shift], "lev", [(i, (i + shift) % BLOCKS) for i in range(BLOCKS)]))
    return moved


def exchanged(to_low, to_high):
    count = lax.axis_size("col")
    forward = [(i, i + 1) for i in range(count - 1)]
    backward = [(b, a) for a, b in forward]
    return lax.ppermute(to_high, "col", forward), lax.ppermute(to_low, "col", backward)


def per_device(control_field, decay_rate, diffusivity):
    field = control_field.reshape(LEVELS * MEMBERS, LONS, LATS)
    local, *pieces, profiles, to_low, to_high = sweep_call(field, decay_rate, diffusivity)
    pieces = shifted(pieces)
    low, high = exchanged(to_low, to_high)
    states = shifted(solve_call(pieces))
    low_s, high_s = exchanged(
        jnp.concatenate([piece[:STATES] for piece in states]),
        jnp.concatenate([piece[STATES : 2 * STATES] for piece in states]),
    )
    whole, begun, kept, spread_rows = inner_call(local, profiles, diffusivity, states)
    out, _ = outer_call(whole, begun, kept, spread_rows, low, high, low_s, high_s)
    return out.reshape(control_field.shape)


def solution(mesh):
    in_specs = (P("lev", None, "col", None), P("lev", "col", None), P("col", None))
    out_specs = P("lev", None, "col", None)
    return jax.shard_map(
        per_device, mesh=mesh, in_specs=in_specs, out_specs=out_specs, check_vma=False
    )
```

```python
import functools

import jax
import jax.numpy as jnp
from jax import lax
from jax.experimental import pallas as pl
from jax.experimental.pallas import tpu as pltpu
from jax.sharding import PartitionSpec as P


SMOOTH = 4
LEVELS = 24
MEMBERS = 16
LONS = 24
LATS = 128
BLOCKS = 4
RECORD = 72
STATES = 64
GROUP = 4
EDGE = (0, 5)
INNER = (1, 2, 3, 4)
SLAB = 8
SLABS = LEVELS // SLAB
PAD = LATS + 16
HALO = GROUP * SLABS * LATS

OFF_CHIP = pl.BlockSpec(memory_space=pltpu.HBM)
ON_CHIP = pl.BlockSpec(memory_space=pltpu.VMEM)
ROOM = pltpu.CompilerParams(vmem_limit_bytes=28 * 2**20)
F32 = jnp.float32


def cost(flops):
    return pl.CostEstimate(flops=flops, transcendentals=0, bytes_accessed=10**6)


def shape(*dims):
    return jax.ShapeDtypeStruct(dims, F32)


def resident(*dims):
    return pltpu.VMEM(dims, F32)


def row(ref, at):
    return ref[pl.ds(at, 8, stride=0), :]


def slot(groups, index, j):
    return 2 * j + index if groups == EDGE else GROUP * index + j


def start_all(copies):
    for copy in copies:
        copy.start()
    return copies


def wait_all(copies):
    for copy in copies:
        copy.wait()


def in_order(pieces, target, rows):
    here = lax.axis_index("lev")
    for shift, piece in enumerate(pieces):
        source = lax.rem(here - shift + BLOCKS, BLOCKS)
        target[pl.ds(pl.multiple_of(source * rows, 8), rows), :] = piece[...]


def responses(rates, profiles, scratch):
    tiles = [slice(8 * tile, 8 * tile + 8) for tile in range(LONS // 8)]
    up, down = range(LEVELS), range(LEVELS - 1, -1, -1)

    def sweep(order, source, target):
        state = [None] * len(tiles)
        for level in order:
            for at, lons in enumerate(tiles):
                rate = rates[level, lons, :]
                if source is None:
                    state[at] = rate if state[at] is None else rate * state[at]
                else:
                    value = (1.0 - rate) * source[level, lons, :]
                    state[at] = value if state[at] is None else rate * state[at] + value
                target[level, lons, :] = state[at]
        return state

    through = sweep(up, None, scratch.at[0])
    sweep(down, None, profiles.at[3])
    q21 = sweep(down, scratch.at[0], profiles.at[2])
    q32 = sweep(up, profiles.at[3], scratch.at[1])
    q31 = sweep(up, profiles.at[2], scratch.at[0])
    q42 = sweep(down, scratch.at[1], profiles.at[1])
    q41 = sweep(down, scratch.at[0], profiles.at[0])
    return through, q21, q31, q32, q41, q42


def sweep_groups(groups, xs, rates, table, local, exits, before):
    values = xs.reshape(LEVELS * MEMBERS * LONS, LATS)
    weights = rates.reshape(LEVELS * LONS, LATS)

    def run(index, carry):
        lon = GROUP * (groups[0] + index * (groups[1] - groups[0]))
        for number in range(4):
            order = range(LEVELS) if number % 2 == 0 else range(LEVELS - 1, -1, -1)
            state = {}
            for level in order:
                for j in range(GROUP):
                    weight = row(weights, level * LONS + lon + j)
                    rest = 1.0 - weight
                    for half in range(2):
                        if number == 0:
                            start = (level * MEMBERS + 8 * half) * LONS + lon + j
                            value = values[pl.ds(start, 8, stride=LONS), :]
                        else:
                            value = local[level, GROUP * index + j, 8 * half : 8 * half + 8, :]
                        value = rest * value
                        if (j, half) in state:
                            value = weight * state[j, half] + value
                        state[j, half] = value
                        local[level, GROUP * index + j, 8 * half : 8 * half + 8, :] = value
            for (j, half), value in state.items():
                place = slot(groups, index, j) * RECORD + 16 * number + 8 * half
                exits[pl.ds(place if isinstance(place, int) else pl.multiple_of(place, 8), 8), :] = value
        return carry

    for index, group in enumerate(groups):
        for j in range(GROUP):
            lon = GROUP * group + j
            for which in range(6):
                record = slot(groups, index, j) * RECORD + STATES + which
                exits[record : record + 1, :] = table[which, lon : lon + 1, :]
    if groups == EDGE:
        for index in range(len(groups)):
            before[index]()
            run(index, 0)
    else:
        lax.fori_loop(0, len(groups), run, 0)


def share_out(exits, pieces, rows):
    here = lax.axis_index("lev")
    for shift, piece in enumerate(pieces):
        target = lax.rem(here + shift, BLOCKS)
        piece[...] = exits[pl.ds(pl.multiple_of(target * rows, 8), rows), :]


def edge_sweep_kernel(field, rate, local, p0, p1, p2, p3, profiles, table, xs, rates, exits, scratch, sems):
    small = pltpu.make_async_copy(rate, rates, sems.at[3])
    small.start()
    loads = {}
    for tile in (0, 2, 1):
        lons = pl.ds(8 * tile, 8)
        loads[tile] = pltpu.make_async_copy(field.at[:, lons, :], xs.at[:, lons, :], sems.at[tile])
        loads[tile].start()
    small.wait()
    for which, tiles in enumerate(responses(rates, profiles, scratch)):
        for tile, value in enumerate(tiles):
            table[which, 8 * tile : 8 * tile + 8, :] = value
    sweep_groups(EDGE, xs, rates, table, local, exits, [loads[0].wait, loads[2].wait])
    share_out(exits, (p0, p1, p2, p3), len(EDGE) * RECORD)
    loads[1].wait()


def edge_sweep_call(field, rate):
    count = GROUP * len(EDGE)
    outs = [resident(LEVELS, count, MEMBERS, LATS)] + [resident(len(EDGE) * RECORD, LATS)] * BLOCKS
    outs += [resident(4, LEVELS, LONS, LATS), resident(6, LONS, LATS), resident(LEVELS * MEMBERS, LONS, LATS), resident(LEVELS, LONS, LATS)]
    return pl.pallas_call(
        edge_sweep_kernel,
        out_shape=outs,
        in_specs=[OFF_CHIP] * 2,
        out_specs=[ON_CHIP] * len(outs),
        scratch_shapes=[
            pltpu.VMEM((count * RECORD, LATS), F32),
            pltpu.VMEM((2, LEVELS, LONS, LATS), F32),
            pltpu.SemaphoreType.DMA((4,)),
        ],
        compiler_params=ROOM,
        cost_estimate=cost(3 * 10**7),
        name="edge_sweeps",
    )(*(pltpu.with_memory_space_constraint(x, pltpu.HBM) for x in (field, rate)))


def inner_sweep_kernel(xs, rates, table, local, p0, p1, p2, p3, exits):
    sweep_groups(INNER, xs, rates, table, local, exits, None)
    share_out(exits, (p0, p1, p2, p3), len(INNER) * RECORD)


def inner_sweep_call(xs, rates, table):
    count = GROUP * len(INNER)
    outs = [resident(LEVELS, count, MEMBERS, LATS)] + [resident(len(INNER) * RECORD, LATS)] * BLOCKS
    return pl.pallas_call(
        inner_sweep_kernel,
        out_shape=outs,
        in_specs=[ON_CHIP] * 3,
        out_specs=[ON_CHIP] * len(outs),
        scratch_shapes=[pltpu.VMEM((count * RECORD, LATS), F32)],
        compiler_params=ROOM,
        cost_estimate=cost(5 * 10**7),
        name="inner_sweeps",
    )(xs, rates, table)


def solve_kernel(share, *refs):
    pieces, outs, (records, states) = refs[:4], refs[4:8], refs[8:]
    in_order(pieces, records, share * RECORD)

    def run(lon, carry):
        def exit_of(block, number, half):
            at = (block * share + lon) * RECORD + 16 * number + 8 * half
            return records[pl.ds(pl.multiple_of(at, 8), 8), :]

        def response(block, which):
            return row(records, (block * share + lon) * RECORD + STATES + which)

        for half in range(2):
            zero = jnp.zeros((8, LATS), F32)
            f1, b1, f2, b2 = ([zero] * BLOCKS for _ in range(4))
            for d in range(BLOCKS - 1):
                f1[d + 1] = exit_of(d, 0, half) + response(d, 0) * f1[d]
            for d in range(BLOCKS - 1, 0, -1):
                b1[d - 1] = exit_of(d, 1, half) + response(d, 1) * f1[d] + response(d, 0) * b1[d]
            for d in range(BLOCKS - 1):
                f2[d + 1] = (
                    exit_of(d, 2, half)
                    + response(d, 2) * f1[d]
                    + response(d, 3) * b1[d]
                    + response(d, 0) * f2[d]
                )
            for d in range(BLOCKS - 1, 0, -1):
                b2[d - 1] = (
                    exit_of(d, 3, half)
                    + response(d, 4) * f1[d]
                    + response(d, 5) * b1[d]
                    + response(d, 1) * f2[d]
                    + response(d, 0) * b2[d]
                )
            for d in range(BLOCKS):
                for number, entering in enumerate((f1, b1, f2, b2)):
                    at = (d * share + lon) * STATES + 16 * number + 8 * half
                    states[pl.ds(pl.multiple_of(at, 8), 8), :] = entering[d]
        return carry

    lax.fori_loop(0, share, run, 0)
    share_out(states, outs, share * STATES)


def solve_call(pieces):
    share = pieces[0].shape[0] // RECORD
    return pl.pallas_call(
        functools.partial(solve_kernel, share),
        out_shape=[resident(share * STATES, LATS)] * BLOCKS,
        in_specs=[ON_CHIP] * BLOCKS,
        out_specs=[ON_CHIP] * BLOCKS,
        scratch_shapes=[
            pltpu.VMEM((BLOCKS * share * RECORD, LATS), F32),
            pltpu.VMEM((BLOCKS * share * STATES, LATS), F32),
        ],
        compiler_params=ROOM,
    )(*pieces)


def corrected_block(value_of, profile_of, entering):
    parts = []
    for level in range(SLAB):
        mine = [profile_of(n, level) for n in range(4)]
        for half in range(2):
            value = value_of(level, half)
            for n in range(4):
                value = value + mine[n] * entering[half][n]
            parts.append(value)
    return jnp.concatenate(parts, axis=0)


def entering_of(states, start):
    return [[states[start + 16 * n + 8 * half : start + 16 * n + 8 * half + 8, :] for n in range(4)] for half in range(2)]


def spread(kappa_row):
    return jnp.transpose(jnp.broadcast_to(kappa_row, (LATS, LATS)))


def stepped(here, around, k):
    return here + k * (around - 4.0 * here)


def clear_pads(rows, blocks):
    zero = jnp.zeros((8, LATS), F32)
    for block in range(blocks):
        rows[block * PAD : block * PAD + 8, :] = zero
        rows[block * PAD + LATS + 8 : (block + 1) * PAD, :] = zero


def edge_kernel(local, profiles, kappa, s0, s1, s2, s3, to_low, to_high, states):
    in_order((s0, s1, s2, s3), states, len(EDGE) * STATES)
    profile_rows = profiles.reshape(4 * LEVELS * LONS, LATS)
    for index, out in enumerate((to_low, to_high)):
        lon = GROUP * EDGE[index]
        out[HALO : HALO + 8, :] = kappa[8 * (lon // 8) : 8 * (lon // 8) + 8, :]

    def run(slab, carry):
        for index, out in enumerate((to_low, to_high)):
            for j in range(GROUP):
                lon = GROUP * EDGE[index] + j
                block = corrected_block(
                    lambda level, half: local[slab * SLAB + level, GROUP * index + j, 8 * half : 8 * half + 8, :],
                    lambda n, level: row(profile_rows, (n * LEVELS + slab * SLAB + level) * LONS + lon),
                    entering_of(states, slot(EDGE, index, j) * STATES),
                )
                out[pl.ds(pl.multiple_of((j * SLABS + slab) * LATS, 8), LATS), :] = jnp.transpose(block)
        return carry

    lax.fori_loop(0, SLABS, run, 0)


def edge_call(local, profiles, diffusivity, pieces):
    return pl.pallas_call(
        edge_kernel,
        out_shape=[resident(HALO + 8, LATS)] * 2,
        in_specs=[ON_CHIP] * 7,
        out_specs=[ON_CHIP] * 2,
        scratch_shapes=[pltpu.VMEM((GROUP * len(EDGE) * STATES, LATS), F32)],
        compiler_params=ROOM,
        cost_estimate=cost(10**7),
        name="edges",
    )(local, profiles, diffusivity, *pieces)


def inner_kernel(local, profiles, kappa, to_low, to_high, s0, s1, s2, s3, out, begun, kept, spread_rows, states, buffers, made, sems):
    def save(slab):
        part = pl.ds(slab * SLAB * MEMBERS, SLAB * MEMBERS)
        return pltpu.make_async_copy(made.at[part], out.at[part, pl.ds(8, 8), :], sems.at[slab])

    in_order((s0, s1, s2, s3), states, len(INNER) * STATES)
    rows = buffers.reshape(2 * LONS * PAD, LATS)
    kept_rows = kept.reshape(SLABS * 2 * 2 * SMOOTH * PAD, LATS)
    clear_pads(rows, 2 * LONS)
    clear_pads(kept_rows, SLABS * 2 * 2 * SMOOTH)
    for lon in range(LONS):
        spread_rows[lon] = spread(kappa[lon : lon + 1, :])
    profile_rows = profiles.reshape(4 * LEVELS * LONS, LATS)
    made_rows = made.reshape(LEVELS * MEMBERS * 8, LATS)
    begun_rows = begun.reshape(2 * LEVELS * MEMBERS * 8, LATS)

    def run(slab, carry):
        def keep(step, lon):
            for side, m in enumerate((lon, LONS - 1 - lon)):
                if step <= m < step + 2 and step < SMOOTH:
                    return ((slab * 2 + side) * 2 * SMOOTH + 2 * step + m - step) * PAD + 8
            return None

        for lon in range(LONS):
            if GROUP <= lon < LONS - GROUP:
                block = jnp.transpose(
                    corrected_block(
                        lambda level, half: local[slab * SLAB + level, lon - GROUP, 8 * half : 8 * half + 8, :],
                        lambda n, level: row(profile_rows, (n * LEVELS + slab * SLAB + level) * LONS + lon),
                        entering_of(states, (lon - GROUP) * STATES),
                    )
                )
            else:
                sent, j = (to_low, lon) if lon < GROUP else (to_high, lon - LONS + GROUP)
                block = sent[pl.ds(pl.multiple_of((j * SLABS + slab) * LATS, 8), LATS), :]
            buffers[0, lon, 8 : 8 + LATS, :] = block
            start = keep(0, lon)
            if start is not None:
                kept_rows[pl.ds(pl.multiple_of(start, 8), LATS), :] = block
        for step in range(SMOOTH):

            def at(which, lon, offset):
                return (which * LONS + lon) * PAD + 8 + offset

            def tile(t, carry):
                source, target = step % 2, (step + 1) % 2
                top = pl.multiple_of(8 * t, 8)
                west = rows[pl.ds(at(source, step, top), 8), :]
                here = rows[pl.ds(at(source, step + 1, top), 8), :]
                for lon in range(step + 1, LONS - step - 1):
                    east = rows[pl.ds(at(source, lon + 1, top), 8), :]
                    north = rows[pl.ds(at(source, lon, top - 1), 8), :]
                    south = rows[pl.ds(at(source, lon, top + 1), 8), :]
                    k = spread_rows[lon, pl.ds(top, 8), :]
                    value = stepped(here, (east + west) + (north + south), k)
                    rows[pl.ds(at(target, lon, top), 8), :] = value
                    start = keep(step + 1, lon)
                    if start is not None:
                        kept_rows[pl.ds(pl.multiple_of(start + top, 8), 8), :] = value
                    west, here = here, east
                return carry

            lax.fori_loop(0, LATS // 8, tile, 0, unroll=2)
        for lon in range(GROUP, LONS - GROUP):
            block = jnp.transpose(buffers[0, lon, 8 : 8 + LATS, :])
            for part in range(2 * SLAB):
                first = slab * SLAB * MEMBERS + 8 * part
                piece = block[8 * part : 8 * part + 8, :]
                if 8 <= lon < 16:
                    made_rows[pl.ds(first * 8 + lon - 8, 8, stride=8), :] = piece
                else:
                    side = lon // 16
                    begun_rows[pl.ds((side * LEVELS * MEMBERS + first) * 8 + lon - 16 * side, 8, stride=8), :] = piece
        save(slab).start()
        return carry

    lax.fori_loop(0, SLABS, run, 0)
    wait_all([save(slab) for slab in range(SLABS)])


def inner_call(local, profiles, diffusivity, to_low, to_high, pieces):
    return pl.pallas_call(
        inner_kernel,
        out_shape=[
            shape(LEVELS * MEMBERS, LONS, LATS),
            resident(2, LEVELS * MEMBERS, 8, LATS),
            resident(SLABS, 2, 2 * SMOOTH, PAD, LATS),
            resident(LONS, LATS, LATS),
        ],
        in_specs=[ON_CHIP] * 9,
        out_specs=[OFF_CHIP, ON_CHIP, ON_CHIP, ON_CHIP],
        scratch_shapes=[
            pltpu.VMEM((GROUP * len(INNER) * STATES, LATS), F32),
            pltpu.VMEM((2, LONS, PAD, LATS), F32),
            pltpu.VMEM((LEVELS * MEMBERS, 8, LATS), F32),
            pltpu.SemaphoreType.DMA((SLABS,)),
        ],
        compiler_params=ROOM,
        cost_estimate=cost(2 * 10**8),
        name="inner",
    )(local, profiles, diffusivity, to_low, to_high, *pieces)


def outer_kernel(whole, begun, kept, spread_rows, low, high, out, filled, buffers, halo_spread, sems):
    places = 2 * SMOOTH

    def saves(slab):
        part = pl.ds(slab * SLAB * MEMBERS, SLAB * MEMBERS)
        return [
            pltpu.make_async_copy(filled.at[side, part], out.at[part, pl.ds(lon, 8), :], sems.at[slab, side])
            for side, lon in enumerate((0, 16))
        ]

    rows = buffers.reshape(2 * 2 * places * PAD, LATS)
    kept_rows = kept.reshape(SLABS * 2 * 2 * SMOOTH * PAD, LATS)
    clear_pads(rows, 2 * 2 * places)
    for side, halo in enumerate((low, high)):
        for j in range(GROUP):
            place = j if side == 0 else GROUP - 1 - j
            at = HALO + (GROUP + j if side == 0 else j)
            halo_spread[side, place] = spread(halo[at : at + 1, :])
    filled_rows = filled.reshape(2 * LEVELS * MEMBERS * 8, LATS)

    def run(slab, carry):
        for side, halo in enumerate((low, high)):
            for j in range(GROUP):
                place = j if side == 0 else GROUP - 1 - j
                block = halo[pl.ds(pl.multiple_of((j * SLABS + slab) * LATS, 8), LATS), :]
                buffers[0, side, place, 8 : 8 + LATS, :] = block
        for step in range(SMOOTH):

            def tile(t, carry):
                top = pl.multiple_of(8 * t, 8)
                for side in range(2):

                    def value_at(place, offset):
                        if place < step + SMOOTH:
                            start = ((step % 2 * 2 + side) * places + place) * PAD
                            return rows[pl.ds(start + 8 + top + offset, 8), :]
                        start = ((slab * 2 + side) * 2 * SMOOTH + 2 * step + place - step - SMOOTH) * PAD
                        return kept_rows[pl.ds(start + 8 + top + offset, 8), :]

                    west, here = value_at(step, 0), value_at(step + 1, 0)
                    for place in range(step + 1, step + SMOOTH + 1):
                        east = value_at(place + 1, 0)
                        around = (east + west) + (value_at(place, -1) + value_at(place, 1))
                        if place < GROUP:
                            k = halo_spread[side, place, pl.ds(top, 8), :]
                        else:
                            m = place - GROUP
                            k = spread_rows[m if side == 0 else LONS - 1 - m, pl.ds(top, 8), :]
                        start = (((step + 1) % 2 * 2 + side) * places + place) * PAD
                        rows[pl.ds(pl.multiple_of(start + 8 + top, 8), 8), :] = stepped(here, around, k)
                        west, here = here, east
                return carry

            lax.fori_loop(0, LATS // 8, tile, 0, unroll=2)
        for side in range(2):
            for m in range(GROUP):
                block = jnp.transpose(buffers[0, side, GROUP + m, 8 : 8 + LATS, :])
                for part in range(2 * SLAB):
                    first = (side * LEVELS + slab * SLAB) * MEMBERS + 8 * part
                    lon = m if side == 0 else 7 - m
                    filled_rows[pl.ds(first * 8 + lon, 8, stride=8), :] = block[8 * part : 8 * part + 8, :]
        start_all(saves(slab))
        return carry

    lax.fori_loop(0, SLABS, run, 0)
    for slab in range(SLABS):
        wait_all(saves(slab))


def outer_call(whole, begun, kept, spread_rows, low, high):
    return pl.pallas_call(
        outer_kernel,
        out_shape=[shape(LEVELS * MEMBERS, LONS, LATS), resident(2, LEVELS * MEMBERS, 8, LATS)],
        in_specs=[OFF_CHIP] + [ON_CHIP] * 5,
        out_specs=[OFF_CHIP, ON_CHIP],
        input_output_aliases={0: 0, 1: 1},
        scratch_shapes=[
            pltpu.VMEM((2, 2, 2 * SMOOTH, PAD, LATS), F32),
            pltpu.VMEM((2, GROUP, LATS, LATS), F32),
            pltpu.SemaphoreType.DMA((SLABS, 2)),
        ],
        compiler_params=ROOM,
        name="outer",
    )(whole, begun, kept, spread_rows, low, high)


def shifted(pieces):
    moved = [pieces[0]]
    for shift in (1, 2, 3):
        moved.append(lax.ppermute(pieces[shift], "lev", [(i, (i + shift) % BLOCKS) for i in range(BLOCKS)]))
    return moved


def exchanged(to_low, to_high):
    count = lax.axis_size("col")
    forward = [(i, i + 1) for i in range(count - 1)]
    backward = [(b, a) for a, b in forward]
    low = lax.ppermute(to_high, "col", forward)
    high = lax.ppermute(to_low, "col", backward)
    return low, high


def per_device(control_field, decay_rate, diffusivity):
    field = control_field.reshape(LEVELS * MEMBERS, LONS, LATS)
    edge_local, *edge_pieces, profiles, table, xs, rates = edge_sweep_call(field, decay_rate)
    inner_local, *inner_pieces = inner_sweep_call(xs, rates, table)
    edge_states = shifted(solve_call(shifted(edge_pieces)))
    inner_states = shifted(solve_call(shifted(inner_pieces)))
    to_low, to_high = edge_call(edge_local, profiles, diffusivity, edge_states)
    low, high = exchanged(to_low, to_high)
    whole, begun, kept, spread_rows = inner_call(inner_local, profiles, diffusivity, to_low, to_high, inner_states)
    out, _ = outer_call(whole, begun, kept, spread_rows, low, high)
    return out.reshape(control_field.shape)


def solution(mesh):
    in_specs = (P("lev", None, "col", None), P("lev", "col", None), P("col", None))
    out_specs = P("lev", None, "col", None)
    return jax.shard_map(
        per_device, mesh=mesh, in_specs=in_specs, out_specs=out_specs, check_vma=False
    )
```

```python
import functools

import jax
import jax.numpy as jnp
from jax import lax
from jax.experimental import pallas as pl
from jax.experimental.pallas import tpu as pltpu
from jax.sharding import PartitionSpec as P


SMOOTH = 4
LEVELS = 24
MEMBERS = 16
LONS = 24
LATS = 128
BLOCKS = 4
PARTNERS = (0, 3, 2, 1)
RECORD = 72
STATES = 64
GROUP = 4
EDGE = (0, 5)
INNER = (1, 2, 3, 4)
SLAB = 8
SLABS = LEVELS // SLAB
PAD = LATS + 24
HALO = GROUP * SLABS * LATS

OFF_CHIP = pl.BlockSpec(memory_space=pltpu.HBM)
ON_CHIP = pl.BlockSpec(memory_space=pltpu.VMEM)
ROOM = pltpu.CompilerParams(vmem_limit_bytes=28 * 2**20)
F32 = jnp.float32


def cost(flops):
    return pl.CostEstimate(flops=flops, transcendentals=0, bytes_accessed=10**6)


def shape(*dims):
    return jax.ShapeDtypeStruct(dims, F32)


def resident(*dims):
    return pltpu.VMEM(dims, F32)


def row(ref, at):
    return ref[pl.ds(at, 8, stride=0), :]


def slot(groups, index, j):
    return 2 * j + index if groups == EDGE else GROUP * index + j


def start_all(copies):
    for copy in copies:
        copy.start()
    return copies


def wait_all(copies):
    for copy in copies:
        copy.wait()


def in_order(pieces, target, rows):
    here = lax.axis_index("lev")
    for mask, piece in zip(PARTNERS, pieces):
        source = jnp.bitwise_xor(here, mask)
        target[pl.ds(pl.multiple_of(source * rows, 8), rows), :] = piece[...]


def responses(rates, profiles, scratch):
    tiles = [slice(8 * tile, 8 * tile + 8) for tile in range(LONS // 8)]
    up, down = range(LEVELS), range(LEVELS - 1, -1, -1)

    def sweep(order, source, target):
        state = [None] * len(tiles)
        for level in order:
            for at, lons in enumerate(tiles):
                rate = rates[level, lons, :]
                if source is None:
                    state[at] = rate if state[at] is None else rate * state[at]
                else:
                    value = (1.0 - rate) * source[level, lons, :]
                    state[at] = value if state[at] is None else rate * state[at] + value
                target[level, lons, :] = state[at]
        return state

    through = sweep(up, None, scratch.at[0])
    sweep(down, None, profiles.at[3])
    q21 = sweep(down, scratch.at[0], profiles.at[2])
    q32 = sweep(up, profiles.at[3], scratch.at[1])
    q31 = sweep(up, profiles.at[2], scratch.at[0])
    q42 = sweep(down, scratch.at[1], profiles.at[1])
    q41 = sweep(down, scratch.at[0], profiles.at[0])
    return through, q21, q31, q32, q41, q42


def sweep_groups(groups, xs, rates, table, local, exits, before):
    values = xs.reshape(LEVELS * MEMBERS * LONS, LATS)
    weights = rates.reshape(LEVELS * LONS, LATS)

    def run(index, carry):
        lon = GROUP * (groups[0] + index * (groups[1] - groups[0]))
        for number in range(4):
            order = range(LEVELS) if number % 2 == 0 else range(LEVELS - 1, -1, -1)
            state = {}
            for level in order:
                for j in range(GROUP):
                    weight = row(weights, level * LONS + lon + j)
                    rest = 1.0 - weight
                    for half in range(2):
                        if number == 0:
                            start = (level * MEMBERS + 8 * half) * LONS + lon + j
                            value = values[pl.ds(start, 8, stride=LONS), :]
                        else:
                            value = local[level, GROUP * index + j, 8 * half : 8 * half + 8, :]
                        value = rest * value
                        if (j, half) in state:
                            value = weight * state[j, half] + value
                        state[j, half] = value
                        local[level, GROUP * index + j, 8 * half : 8 * half + 8, :] = value
            for (j, half), value in state.items():
                place = slot(groups, index, j) * RECORD + 16 * number + 8 * half
                exits[pl.ds(place if isinstance(place, int) else pl.multiple_of(place, 8), 8), :] = value
        return carry

    for index, group in enumerate(groups):
        for j in range(GROUP):
            lon = GROUP * group + j
            for which in range(6):
                record = slot(groups, index, j) * RECORD + STATES + which
                exits[record : record + 1, :] = table[which, lon : lon + 1, :]
    if groups == EDGE:
        for index in range(len(groups)):
            before[index]()
            run(index, 0)
    else:
        lax.fori_loop(0, len(groups), run, 0)


def share_out(exits, pieces, rows):
    here = lax.axis_index("lev")
    for mask, piece in zip(PARTNERS, pieces):
        target = jnp.bitwise_xor(here, mask)
        piece[...] = exits[pl.ds(pl.multiple_of(target * rows, 8), rows), :]


def edge_sweep_kernel(field, rate, local, p0, p1, p2, p3, profiles, table, xs, rates, exits, scratch, sems):
    small = pltpu.make_async_copy(rate, rates, sems.at[3])
    small.start()
    loads = {}
    for tile in (0, 2, 1):
        lons = pl.ds(8 * tile, 8)
        loads[tile] = pltpu.make_async_copy(field.at[:, lons, :], xs.at[:, lons, :], sems.at[tile])
        loads[tile].start()
    small.wait()
    for which, tiles in enumerate(responses(rates, profiles, scratch)):
        for tile, value in enumerate(tiles):
            table[which, 8 * tile : 8 * tile + 8, :] = value
    sweep_groups(EDGE, xs, rates, table, local, exits, [loads[0].wait, loads[2].wait])
    share_out(exits, (p0, p1, p2, p3), len(EDGE) * RECORD)
    loads[1].wait()


def edge_sweep_call(field, rate):
    count = GROUP * len(EDGE)
    outs = [resident(LEVELS, count, MEMBERS, LATS)] + [resident(len(EDGE) * RECORD, LATS)] * BLOCKS
    outs += [resident(4, LEVELS, LONS, LATS), resident(6, LONS, LATS), resident(LEVELS * MEMBERS, LONS, LATS), resident(LEVELS, LONS, LATS)]
    return pl.pallas_call(
        edge_sweep_kernel,
        out_shape=outs,
        in_specs=[OFF_CHIP] * 2,
        out_specs=[ON_CHIP] * len(outs),
        scratch_shapes=[
            pltpu.VMEM((count * RECORD, LATS), F32),
            pltpu.VMEM((2, LEVELS, LONS, LATS), F32),
            pltpu.SemaphoreType.DMA((4,)),
        ],
        compiler_params=ROOM,
        cost_estimate=cost(3 * 10**7),
        name="edge_sweeps",
    )(*(pltpu.with_memory_space_constraint(x, pltpu.HBM) for x in (field, rate)))


def inner_sweep_kernel(xs, rates, table, local, p0, p1, p2, p3, exits):
    sweep_groups(INNER, xs, rates, table, local, exits, None)
    share_out(exits, (p0, p1, p2, p3), len(INNER) * RECORD)


def inner_sweep_call(xs, rates, table):
    count = GROUP * len(INNER)
    outs = [resident(LEVELS, count, MEMBERS, LATS)] + [resident(len(INNER) * RECORD, LATS)] * BLOCKS
    return pl.pallas_call(
        inner_sweep_kernel,
        out_shape=outs,
        in_specs=[ON_CHIP] * 3,
        out_specs=[ON_CHIP] * len(outs),
        scratch_shapes=[pltpu.VMEM((count * RECORD, LATS), F32)],
        compiler_params=ROOM,
        cost_estimate=cost(5 * 10**7),
        name="inner_sweeps",
    )(xs, rates, table)


def solve_kernel(share, *refs):
    pieces, outs, (records, states) = refs[:4], refs[4:8], refs[8:]
    in_order(pieces, records, share * RECORD)

    def run(lon, carry):
        def exit_of(block, number, half):
            at = (block * share + lon) * RECORD + 16 * number + 8 * half
            return records[pl.ds(pl.multiple_of(at, 8), 8), :]

        def response(block, which):
            return row(records, (block * share + lon) * RECORD + STATES + which)

        for half in range(2):
            zero = jnp.zeros((8, LATS), F32)
            f1, b1, f2, b2 = ([zero] * BLOCKS for _ in range(4))
            for d in range(BLOCKS - 1):
                f1[d + 1] = exit_of(d, 0, half) + response(d, 0) * f1[d]
            for d in range(BLOCKS - 1, 0, -1):
                b1[d - 1] = exit_of(d, 1, half) + response(d, 1) * f1[d] + response(d, 0) * b1[d]
            for d in range(BLOCKS - 1):
                f2[d + 1] = (
                    exit_of(d, 2, half)
                    + response(d, 2) * f1[d]
                    + response(d, 3) * b1[d]
                    + response(d, 0) * f2[d]
                )
            for d in range(BLOCKS - 1, 0, -1):
                b2[d - 1] = (
                    exit_of(d, 3, half)
                    + response(d, 4) * f1[d]
                    + response(d, 5) * b1[d]
                    + response(d, 1) * f2[d]
                    + response(d, 0) * b2[d]
                )
            for d in range(BLOCKS):
                for number, entering in enumerate((f1, b1, f2, b2)):
                    at = (d * share + lon) * STATES + 16 * number + 8 * half
                    states[pl.ds(pl.multiple_of(at, 8), 8), :] = entering[d]
        return carry

    lax.fori_loop(0, share, run, 0)
    share_out(states, outs, share * STATES)


def solve_call(pieces):
    share = pieces[0].shape[0] // RECORD
    return pl.pallas_call(
        functools.partial(solve_kernel, share),
        out_shape=[resident(share * STATES, LATS)] * BLOCKS,
        in_specs=[ON_CHIP] * BLOCKS,
        out_specs=[ON_CHIP] * BLOCKS,
        scratch_shapes=[
            pltpu.VMEM((BLOCKS * share * RECORD, LATS), F32),
            pltpu.VMEM((BLOCKS * share * STATES, LATS), F32),
        ],
        compiler_params=ROOM,
    )(*pieces)


def corrected_block(value_of, profile_of, entering):
    parts = []
    for level in range(SLAB):
        mine = [profile_of(n, level) for n in range(4)]
        for half in range(2):
            value = value_of(level, half)
            for n in range(4):
                value = value + mine[n] * entering[half][n]
            parts.append(value)
    return jnp.concatenate(parts, axis=0)


def entering_of(states, start):
    return [[states[pl.ds(start + 16 * n + 8 * half, 8), :] for n in range(4)] for half in range(2)]


def spread(kappa_row):
    return jnp.transpose(jnp.broadcast_to(kappa_row, (LATS, LATS)))


def by_core(act, mate, other):
    odd = lax.rem(lax.axis_index("col"), 2)
    pl.when(odd == 0)(lambda: act(other, mate))
    pl.when(odd == 1)(lambda: act(mate, other))


def stepped(here, around, k):
    return here + k * (around - 4.0 * here)


def clear_pads(rows, blocks):
    zero = jnp.zeros((8, LATS), F32)
    for block in range(blocks):
        rows[block * PAD : block * PAD + 8, :] = zero
        rows[block * PAD + LATS + 8 : block * PAD + LATS + 16, :] = zero


def edge_kernel(local, profiles, kappa, s0, s1, s2, s3, to_mate, to_other, states):
    odd = lax.rem(lax.axis_index("col"), 2)
    in_order((s0, s1, s2, s3), states, len(EDGE) * STATES)
    profile_rows = profiles.reshape(4 * LEVELS * LONS, LATS)
    sides = ((to_mate, 1 - odd), (to_other, odd))
    for out, index in sides:
        out[HALO : HALO + 8, :] = kappa[pl.ds(pl.multiple_of(16 * index, 8), 8), :]

    def run(slab, carry):
        for out, index in sides:
            for j in range(GROUP):
                lon = GROUP * (EDGE[1] - EDGE[0]) * index + j
                block = corrected_block(
                    lambda level, half: local[slab * SLAB + level, GROUP * index + j, 8 * half : 8 * half + 8, :],
                    lambda n, level: row(profile_rows, (n * LEVELS + slab * SLAB + level) * LONS + lon),
                    entering_of(states, pl.multiple_of(slot(EDGE, index, j) * STATES, 8)),
                )
                out[pl.ds(pl.multiple_of((j * SLABS + slab) * LATS, 8), LATS), :] = jnp.transpose(block)
        return carry

    lax.fori_loop(0, SLABS, run, 0)


def edge_call(local, profiles, diffusivity, pieces):
    return pl.pallas_call(
        edge_kernel,
        out_shape=[resident(HALO + 8, LATS)] * 2,
        in_specs=[ON_CHIP] * 7,
        out_specs=[ON_CHIP] * 2,
        scratch_shapes=[pltpu.VMEM((GROUP * len(EDGE) * STATES, LATS), F32)],
        compiler_params=ROOM,
        cost_estimate=cost(10**7),
        name="edges",
    )(local, profiles, diffusivity, *pieces)


def inner_kernel(local, profiles, kappa, to_mate, to_other, s0, s1, s2, s3, out, begun, kept, spread_rows, states, buffers, made, sems):
    def save(slab):
        part = pl.ds(slab * SLAB * MEMBERS, SLAB * MEMBERS)
        return pltpu.make_async_copy(made.at[part], out.at[part, pl.ds(8, 8), :], sems.at[slab])

    in_order((s0, s1, s2, s3), states, len(INNER) * STATES)
    rows = buffers.reshape(2 * LONS * PAD, LATS)
    kept_rows = kept.reshape(SLABS * 2 * 2 * SMOOTH * PAD, LATS)
    clear_pads(rows, 2 * LONS)
    clear_pads(kept_rows, SLABS * 2 * 2 * SMOOTH)
    for lon in range(LONS):
        spread_rows[lon] = spread(kappa[lon : lon + 1, :])
    profile_rows = profiles.reshape(4 * LEVELS * LONS, LATS)
    made_rows = made.reshape(LEVELS * MEMBERS * 8, LATS)
    begun_rows = begun.reshape(2 * LEVELS * MEMBERS * 8, LATS)

    def run(slab, carry):
        def keep(step, lon):
            for side, m in enumerate((lon, LONS - 1 - lon)):
                if step <= m < step + 2 and step < SMOOTH:
                    return ((slab * 2 + side) * 2 * SMOOTH + 2 * step + m - step) * PAD + 8
            return None

        for lon in range(GROUP, LONS - GROUP):
            block = corrected_block(
                lambda level, half: local[slab * SLAB + level, lon - GROUP, 8 * half : 8 * half + 8, :],
                lambda n, level: row(profile_rows, (n * LEVELS + slab * SLAB + level) * LONS + lon),
                entering_of(states, (lon - GROUP) * STATES),
            )
            buffers[0, lon, 8 : 8 + LATS, :] = jnp.transpose(block)

        def edges(to_low, to_high):
            for index, sent in enumerate((to_low, to_high)):
                for j in range(GROUP):
                    lon = GROUP * EDGE[index] + j
                    block = sent[pl.ds(pl.multiple_of((j * SLABS + slab) * LATS, 8), LATS), :]
                    buffers[0, lon, 8 : 8 + LATS, :] = block
                    start = keep(0, lon)
                    if start is not None:
                        kept_rows[pl.ds(pl.multiple_of(start, 8), LATS), :] = block

        by_core(edges, to_mate, to_other)
        for step in range(SMOOTH):

            def at(which, lon, offset):
                return (which * LONS + lon) * PAD + 8 + offset

            def tile(t, carry):
                source, target = step % 2, (step + 1) % 2
                top = pl.multiple_of(8 * t, 8)
                west = rows[pl.ds(at(source, step, top), 8), :]
                here = rows[pl.ds(at(source, step + 1, top), 8), :]
                for lon in range(step + 1, LONS - step - 1):
                    east = rows[pl.ds(at(source, lon + 1, top), 8), :]
                    north = rows[pl.ds(at(source, lon, top - 1), 8), :]
                    south = rows[pl.ds(at(source, lon, top + 1), 8), :]
                    k = spread_rows[lon, pl.ds(top, 8), :]
                    value = stepped(here, (east + west) + (north + south), k)
                    rows[pl.ds(at(target, lon, top), 8), :] = value
                    start = keep(step + 1, lon)
                    if start is not None:
                        kept_rows[pl.ds(pl.multiple_of(start + top, 8), 8), :] = value
                    west, here = here, east
                return carry

            lax.fori_loop(0, LATS // 8, tile, 0, unroll=4)
        for lon in range(GROUP, LONS - GROUP):
            block = jnp.transpose(buffers[0, lon, 8 : 8 + LATS, :])
            for part in range(2 * SLAB):
                first = slab * SLAB * MEMBERS + 8 * part
                piece = block[8 * part : 8 * part + 8, :]
                if 8 <= lon < 16:
                    made_rows[pl.ds(first * 8 + lon - 8, 8, stride=8), :] = piece
                else:
                    side = lon // 16
                    begun_rows[pl.ds((side * LEVELS * MEMBERS + first) * 8 + lon - 16 * side, 8, stride=8), :] = piece
        save(slab).start()
        return carry

    lax.fori_loop(0, SLABS, run, 0)
    wait_all([save(slab) for slab in range(SLABS)])


def inner_call(local, profiles, diffusivity, to_mate, to_other, pieces):
    return pl.pallas_call(
        inner_kernel,
        out_shape=[
            shape(LEVELS * MEMBERS, LONS, LATS),
            resident(2, LEVELS * MEMBERS, 8, LATS),
            resident(SLABS, 2, 2 * SMOOTH, PAD, LATS),
            resident(LONS, LATS, LATS),
        ],
        in_specs=[ON_CHIP] * 9,
        out_specs=[OFF_CHIP, ON_CHIP, ON_CHIP, ON_CHIP],
        scratch_shapes=[
            pltpu.VMEM((GROUP * len(INNER) * STATES, LATS), F32),
            pltpu.VMEM((2, LONS, PAD, LATS), F32),
            pltpu.VMEM((LEVELS * MEMBERS, 8, LATS), F32),
            pltpu.SemaphoreType.DMA((SLABS,)),
        ],
        compiler_params=ROOM,
        cost_estimate=cost(2 * 10**8),
        name="inner",
    )(local, profiles, diffusivity, to_mate, to_other, *pieces)


def outer_kernel(whole, begun, kept, spread_rows, mate, other, out, filled, buffers, halo_spread, sems):
    places = 2 * SMOOTH

    def saves(slab):
        part = pl.ds(slab * SLAB * MEMBERS, SLAB * MEMBERS)
        return [
            pltpu.make_async_copy(filled.at[side, part], out.at[part, pl.ds(lon, 8), :], sems.at[slab, side])
            for side, lon in enumerate((0, 16))
        ]

    rows = buffers.reshape(2 * 2 * places * PAD, LATS)
    kept_rows = kept.reshape(SLABS * 2 * 2 * SMOOTH * PAD, LATS)
    clear_pads(rows, 2 * 2 * places)

    def spreads(low, high):
        for side, halo in enumerate((low, high)):
            for j in range(GROUP):
                place = j if side == 0 else GROUP - 1 - j
                at = HALO + (GROUP + j if side == 0 else j)
                halo_spread[side, place] = spread(halo[at : at + 1, :])

    by_core(spreads, mate, other)
    filled_rows = filled.reshape(2 * LEVELS * MEMBERS * 8, LATS)

    def run(slab, carry):
        def halos(low, high):
            for side, halo in enumerate((low, high)):
                for j in range(GROUP):
                    place = j if side == 0 else GROUP - 1 - j
                    block = halo[pl.ds(pl.multiple_of((j * SLABS + slab) * LATS, 8), LATS), :]
                    buffers[0, side, place, 8 : 8 + LATS, :] = block

        by_core(halos, mate, other)
        for step in range(SMOOTH):

            def tile(t, carry):
                top = pl.multiple_of(8 * t, 8)
                for side in range(2):

                    def value_at(place, offset):
                        if place < step + SMOOTH:
                            start = ((step % 2 * 2 + side) * places + place) * PAD
                            return rows[pl.ds(start + 8 + top + offset, 8), :]
                        start = ((slab * 2 + side) * 2 * SMOOTH + 2 * step + place - step - SMOOTH) * PAD
                        return kept_rows[pl.ds(start + 8 + top + offset, 8), :]

                    west, here = value_at(step, 0), value_at(step + 1, 0)
                    for place in range(step + 1, step + SMOOTH + 1):
                        east = value_at(place + 1, 0)
                        around = (east + west) + (value_at(place, -1) + value_at(place, 1))
                        if place < GROUP:
                            k = halo_spread[side, place, pl.ds(top, 8), :]
                        else:
                            m = place - GROUP
                            k = spread_rows[m if side == 0 else LONS - 1 - m, pl.ds(top, 8), :]
                        start = (((step + 1) % 2 * 2 + side) * places + place) * PAD
                        rows[pl.ds(pl.multiple_of(start + 8 + top, 8), 8), :] = stepped(here, around, k)
                        west, here = here, east
                return carry

            lax.fori_loop(0, LATS // 8, tile, 0, unroll=4)
        for side in range(2):
            for m in range(GROUP):
                block = jnp.transpose(buffers[0, side, GROUP + m, 8 : 8 + LATS, :])
                for part in range(2 * SLAB):
                    first = (side * LEVELS + slab * SLAB) * MEMBERS + 8 * part
                    lon = m if side == 0 else 7 - m
                    filled_rows[pl.ds(first * 8 + lon, 8, stride=8), :] = block[8 * part : 8 * part + 8, :]
        start_all(saves(slab))
        return carry

    lax.fori_loop(0, SLABS, run, 0)
    for slab in range(SLABS):
        wait_all(saves(slab))


def outer_call(whole, begun, kept, spread_rows, mate, other):
    return pl.pallas_call(
        outer_kernel,
        out_shape=[shape(LEVELS * MEMBERS, LONS, LATS), resident(2, LEVELS * MEMBERS, 8, LATS)],
        in_specs=[OFF_CHIP] + [ON_CHIP] * 5,
        out_specs=[OFF_CHIP, ON_CHIP],
        input_output_aliases={0: 0, 1: 1},
        scratch_shapes=[
            pltpu.VMEM((2, 2, 2 * SMOOTH, PAD, LATS), F32),
            pltpu.VMEM((2, GROUP, LATS, LATS), F32),
            pltpu.SemaphoreType.DMA((SLABS, 2)),
        ],
        compiler_params=ROOM,
        name="outer",
    )(whole, begun, kept, spread_rows, mate, other)


def shifted(pieces):
    moved = [pieces[0]]
    for at in (1, 2, 3):
        moved.append(lax.ppermute(pieces[at], "lev", [(i, i ^ PARTNERS[at]) for i in range(BLOCKS)]))
    return moved


def exchanged(to_mate, to_other):
    count = lax.axis_size("col")
    both_ways = lambda first: [pair for i in range(first, count - 1, 2) for pair in ((i, i + 1), (i + 1, i))]
    mate = lax.ppermute(to_mate, "col", both_ways(0))
    other = lax.ppermute(to_other, "col", both_ways(1))
    return mate, other


def per_device(control_field, decay_rate, diffusivity):
    field = control_field.reshape(LEVELS * MEMBERS, LONS, LATS)
    edge_local, *edge_pieces, profiles, table, xs, rates = edge_sweep_call(field, decay_rate)
    inner_local, *inner_pieces = inner_sweep_call(xs, rates, table)
    edge_states = shifted(solve_call(shifted(edge_pieces)))
    inner_states = shifted(solve_call(shifted(inner_pieces)))
    to_mate, to_other = edge_call(edge_local, profiles, diffusivity, edge_states)
    mate, other = exchanged(to_mate, to_other)
    whole, begun, kept, spread_rows = inner_call(inner_local, profiles, diffusivity, to_mate, to_other, inner_states)
    out, _ = outer_call(whole, begun, kept, spread_rows, mate, other)
    return out.reshape(control_field.shape)


def solution(mesh):
    in_specs = (P("lev", None, "col", None), P("lev", "col", None), P("col", None))
    out_specs = P("lev", None, "col", None)
    return jax.shard_map(
        per_device, mesh=mesh, in_specs=in_specs, out_specs=out_specs, check_vma=False
    )
```

```python
import functools

import jax
import jax.numpy as jnp
from jax import lax
from jax.experimental import pallas as pl
from jax.experimental.pallas import tpu as pltpu
from jax.sharding import PartitionSpec as P


SMOOTH = 4
LEVELS = 24
MEMBERS = 16
LONS = 24
LATS = 128
BLOCKS = 4
PARTNERS = (0, 3, 2, 1)
RECORD = 72
STATES = 64
GROUP = 4
EDGE = ((0, 1, 2, 3), (20, 21, 22, 23), (4, 5, 18, 19))
INNER = ((6, 7, 8, 9), (10, 11, 12, 13), (14, 15, 16, 17))
SENT = 2
SLAB = 8
SLABS = LEVELS // SLAB
PAD = LATS + 24
HALO = GROUP * SLABS * LATS

OFF_CHIP = pl.BlockSpec(memory_space=pltpu.HBM)
ON_CHIP = pl.BlockSpec(memory_space=pltpu.VMEM)
ROOM = pltpu.CompilerParams(vmem_limit_bytes=28 * 2**20)
F32 = jnp.float32


def cost(flops):
    return pl.CostEstimate(flops=flops, transcendentals=0, bytes_accessed=10**6)


def shape(*dims):
    return jax.ShapeDtypeStruct(dims, F32)


def resident(*dims):
    return pltpu.VMEM(dims, F32)


def row(ref, at):
    return ref[pl.ds(at, 8, stride=0), :]


def slot(groups, index, j):
    return len(groups) * j + index if groups == EDGE else GROUP * index + j


def start_all(copies):
    for copy in copies:
        copy.start()
    return copies


def wait_all(copies):
    for copy in copies:
        copy.wait()


def in_order(pieces, target, rows):
    here = lax.axis_index("lev")
    for mask, piece in zip(PARTNERS, pieces):
        source = jnp.bitwise_xor(here, mask)
        target[pl.ds(pl.multiple_of(source * rows, 8), rows), :] = piece[...]


def responses(rates, profiles, scratch):
    tiles = [slice(8 * tile, 8 * tile + 8) for tile in range(LONS // 8)]
    up, down = range(LEVELS), range(LEVELS - 1, -1, -1)

    def sweep(order, source, target):
        state = [None] * len(tiles)
        for level in order:
            for at, lons in enumerate(tiles):
                rate = rates[level, lons, :]
                if source is None:
                    state[at] = rate if state[at] is None else rate * state[at]
                else:
                    value = (1.0 - rate) * source[level, lons, :]
                    state[at] = value if state[at] is None else rate * state[at] + value
                target[level, lons, :] = state[at]
        return state

    through = sweep(up, None, scratch.at[0])
    sweep(down, None, profiles.at[3])
    q21 = sweep(down, scratch.at[0], profiles.at[2])
    q32 = sweep(up, profiles.at[3], scratch.at[1])
    q31 = sweep(up, profiles.at[2], scratch.at[0])
    q42 = sweep(down, scratch.at[1], profiles.at[1])
    q41 = sweep(down, scratch.at[0], profiles.at[0])
    return through, q21, q31, q32, q41, q42


def sweep_groups(groups, xs, rates, table, local, exits, before):
    values = xs.reshape(LEVELS * MEMBERS * LONS, LATS)
    weights = rates.reshape(LEVELS * LONS, LATS)

    def run(index, carry):
        lons = groups[index] if isinstance(index, int) else [groups[0][0] + GROUP * index + j for j in range(GROUP)]
        for number in range(4):
            order = range(LEVELS) if number % 2 == 0 else range(LEVELS - 1, -1, -1)
            state = {}
            for level in order:
                for j in range(GROUP):
                    weight = row(weights, level * LONS + lons[j])
                    rest = 1.0 - weight
                    for half in range(2):
                        if number == 0:
                            start = (level * MEMBERS + 8 * half) * LONS + lons[j]
                            value = values[pl.ds(start, 8, stride=LONS), :]
                        else:
                            value = local[level, GROUP * index + j, 8 * half : 8 * half + 8, :]
                        value = rest * value
                        if (j, half) in state:
                            value = weight * state[j, half] + value
                        state[j, half] = value
                        local[level, GROUP * index + j, 8 * half : 8 * half + 8, :] = value
            for (j, half), value in state.items():
                place = slot(groups, index, j) * RECORD + 16 * number + 8 * half
                exits[pl.ds(place if isinstance(place, int) else pl.multiple_of(place, 8), 8), :] = value
        return carry

    for index, group in enumerate(groups):
        for j in range(GROUP):
            lon = group[j]
            for which in range(6):
                record = slot(groups, index, j) * RECORD + STATES + which
                exits[record : record + 1, :] = table[which, lon : lon + 1, :]
    if groups == EDGE:
        for index in range(len(groups)):
            before[index]()
            run(index, 0)
    else:
        lax.fori_loop(0, len(groups), run, 0)


def share_out(exits, pieces, rows):
    here = lax.axis_index("lev")
    for mask, piece in zip(PARTNERS, pieces):
        target = jnp.bitwise_xor(here, mask)
        piece[...] = exits[pl.ds(pl.multiple_of(target * rows, 8), rows), :]


def edge_sweep_kernel(field, rate, local, p0, p1, p2, p3, profiles, table, xs, rates, exits, scratch, sems):
    small = pltpu.make_async_copy(rate, rates, sems.at[3])
    small.start()
    loads = {}
    for tile in (0, 2, 1):
        lons = pl.ds(8 * tile, 8)
        loads[tile] = pltpu.make_async_copy(field.at[:, lons, :], xs.at[:, lons, :], sems.at[tile])
        loads[tile].start()
    small.wait()
    for which, tiles in enumerate(responses(rates, profiles, scratch)):
        for tile, value in enumerate(tiles):
            table[which, 8 * tile : 8 * tile + 8, :] = value
    sweep_groups(EDGE, xs, rates, table, local, exits, [loads[0].wait, loads[2].wait, lambda: None])
    share_out(exits, (p0, p1, p2, p3), len(EDGE) * RECORD)
    loads[1].wait()


def edge_sweep_call(field, rate):
    count = GROUP * len(EDGE)
    outs = [resident(LEVELS, count, MEMBERS, LATS)] + [resident(len(EDGE) * RECORD, LATS)] * BLOCKS
    outs += [resident(4, LEVELS, LONS, LATS), resident(6, LONS, LATS), resident(LEVELS * MEMBERS, LONS, LATS), resident(LEVELS, LONS, LATS)]
    return pl.pallas_call(
        edge_sweep_kernel,
        out_shape=outs,
        in_specs=[OFF_CHIP] * 2,
        out_specs=[ON_CHIP] * len(outs),
        scratch_shapes=[
            pltpu.VMEM((count * RECORD, LATS), F32),
            pltpu.VMEM((2, LEVELS, LONS, LATS), F32),
            pltpu.SemaphoreType.DMA((4,)),
        ],
        compiler_params=ROOM,
        cost_estimate=cost(3 * 10**7),
        name="edge_sweeps",
    )(*(pltpu.with_memory_space_constraint(x, pltpu.HBM) for x in (field, rate)))


def inner_sweep_kernel(xs, rates, table, local, p0, p1, p2, p3, exits):
    sweep_groups(INNER, xs, rates, table, local, exits, None)
    share_out(exits, (p0, p1, p2, p3), len(INNER) * RECORD)


def inner_sweep_call(xs, rates, table):
    count = GROUP * len(INNER)
    outs = [resident(LEVELS, count, MEMBERS, LATS)] + [resident(len(INNER) * RECORD, LATS)] * BLOCKS
    return pl.pallas_call(
        inner_sweep_kernel,
        out_shape=outs,
        in_specs=[ON_CHIP] * 3,
        out_specs=[ON_CHIP] * len(outs),
        scratch_shapes=[pltpu.VMEM((count * RECORD, LATS), F32)],
        compiler_params=ROOM,
        cost_estimate=cost(5 * 10**7),
        name="inner_sweeps",
    )(xs, rates, table)


def solve_kernel(share, *refs):
    pieces, outs, (records, states) = refs[:4], refs[4:8], refs[8:]
    in_order(pieces, records, share * RECORD)

    def run(lon, carry):
        def exit_of(block, number, half):
            at = (block * share + lon) * RECORD + 16 * number + 8 * half
            return records[pl.ds(pl.multiple_of(at, 8), 8), :]

        def response(block, which):
            return row(records, (block * share + lon) * RECORD + STATES + which)

        for half in range(2):
            zero = jnp.zeros((8, LATS), F32)
            f1, b1, f2, b2 = ([zero] * BLOCKS for _ in range(4))
            for d in range(BLOCKS - 1):
                f1[d + 1] = exit_of(d, 0, half) + response(d, 0) * f1[d]
            for d in range(BLOCKS - 1, 0, -1):
                b1[d - 1] = exit_of(d, 1, half) + response(d, 1) * f1[d] + response(d, 0) * b1[d]
            for d in range(BLOCKS - 1):
                f2[d + 1] = (
                    exit_of(d, 2, half)
                    + response(d, 2) * f1[d]
                    + response(d, 3) * b1[d]
                    + response(d, 0) * f2[d]
                )
            for d in range(BLOCKS - 1, 0, -1):
                b2[d - 1] = (
                    exit_of(d, 3, half)
                    + response(d, 4) * f1[d]
                    + response(d, 5) * b1[d]
                    + response(d, 1) * f2[d]
                    + response(d, 0) * b2[d]
                )
            for d in range(BLOCKS):
                for number, entering in enumerate((f1, b1, f2, b2)):
                    at = (d * share + lon) * STATES + 16 * number + 8 * half
                    states[pl.ds(pl.multiple_of(at, 8), 8), :] = entering[d]
        return carry

    lax.fori_loop(0, share, run, 0)
    share_out(states, outs, share * STATES)


def solve_call(pieces):
    share = pieces[0].shape[0] // RECORD
    return pl.pallas_call(
        functools.partial(solve_kernel, share),
        out_shape=[resident(share * STATES, LATS)] * BLOCKS,
        in_specs=[ON_CHIP] * BLOCKS,
        out_specs=[ON_CHIP] * BLOCKS,
        scratch_shapes=[
            pltpu.VMEM((BLOCKS * share * RECORD, LATS), F32),
            pltpu.VMEM((BLOCKS * share * STATES, LATS), F32),
        ],
        compiler_params=ROOM,
    )(*pieces)


def corrected_block(value_of, profile_of, entering):
    parts = []
    for level in range(SLAB):
        mine = [profile_of(n, level) for n in range(4)]
        for half in range(2):
            value = value_of(level, half)
            for n in range(4):
                value = value + mine[n] * entering[half][n]
            parts.append(value)
    return jnp.concatenate(parts, axis=0)


def entering_of(states, start):
    return [[states[pl.ds(start + 16 * n + 8 * half, 8), :] for n in range(4)] for half in range(2)]


def spread(kappa_row):
    return jnp.transpose(jnp.broadcast_to(kappa_row, (LATS, LATS)))


def by_core(act, mate, other):
    odd = lax.rem(lax.axis_index("col"), 2)
    pl.when(odd == 0)(lambda: act(other, mate))
    pl.when(odd == 1)(lambda: act(mate, other))


def stepped(here, around, k):
    return here + k * (around - 4.0 * here)


def clear_pads(rows, blocks):
    zero = jnp.zeros((8, LATS), F32)
    for block in range(blocks):
        rows[block * PAD : block * PAD + 8, :] = zero
        rows[block * PAD + LATS + 8 : block * PAD + LATS + 16, :] = zero


def edge_kernel(local, profiles, kappa, s0, s1, s2, s3, to_mate, to_other, states):
    odd = lax.rem(lax.axis_index("col"), 2)
    in_order((s0, s1, s2, s3), states, len(EDGE) * STATES)
    profile_rows = profiles.reshape(4 * LEVELS * LONS, LATS)
    sides = ((to_mate, 1 - odd), (to_other, odd))
    for out, index in sides:
        out[HALO : HALO + 8, :] = kappa[pl.ds(pl.multiple_of(16 * index, 8), 8), :]

    def run(slab, carry):
        for out, index in sides:
            for j in range(GROUP):
                lon = (LONS - GROUP) * index + j
                block = corrected_block(
                    lambda level, half: local[slab * SLAB + level, GROUP * index + j, 8 * half : 8 * half + 8, :],
                    lambda n, level: row(profile_rows, (n * LEVELS + slab * SLAB + level) * LONS + lon),
                    entering_of(states, pl.multiple_of(slot(EDGE, index, j) * STATES, 8)),
                )
                out[pl.ds(pl.multiple_of((j * SLABS + slab) * LATS, 8), LATS), :] = jnp.transpose(block)
        return carry

    lax.fori_loop(0, SLABS, run, 0)


def edge_call(local, profiles, diffusivity, pieces):
    return pl.pallas_call(
        edge_kernel,
        out_shape=[resident(HALO + 8, LATS)] * 2,
        in_specs=[ON_CHIP] * 7,
        out_specs=[ON_CHIP] * 2,
        scratch_shapes=[pltpu.VMEM((GROUP * len(EDGE) * STATES, LATS), F32)],
        compiler_params=ROOM,
        cost_estimate=cost(10**7),
        name="edges",
    )(local, profiles, diffusivity, *pieces)


def inner_kernel(local, edge_local, profiles, kappa, to_mate, to_other, *refs):
    pieces, edge_pieces, refs = refs[:4], refs[4:8], refs[8:]
    out, begun, kept, spread_rows, states, edge_states, buffers, made, sems = refs

    def save(slab):
        part = pl.ds(slab * SLAB * MEMBERS, SLAB * MEMBERS)
        return pltpu.make_async_copy(made.at[part], out.at[part, pl.ds(8, 8), :], sems.at[slab])

    in_order(pieces, states, len(INNER) * STATES)
    in_order(edge_pieces, edge_states, len(EDGE) * STATES)
    rows = buffers.reshape(2 * LONS * PAD, LATS)
    kept_rows = kept.reshape(SLABS * 2 * 2 * SMOOTH * PAD, LATS)
    clear_pads(rows, 2 * LONS)
    clear_pads(kept_rows, SLABS * 2 * 2 * SMOOTH)
    for lon in range(LONS):
        spread_rows[lon] = spread(kappa[lon : lon + 1, :])
    profile_rows = profiles.reshape(4 * LEVELS * LONS, LATS)
    made_rows = made.reshape(LEVELS * MEMBERS * 8, LATS)
    begun_rows = begun.reshape(2 * LEVELS * MEMBERS * 8, LATS)

    def run(slab, carry):
        def keep(step, lon):
            for side, m in enumerate((lon, LONS - 1 - lon)):
                if step <= m < step + 2 and step < SMOOTH:
                    return ((slab * 2 + side) * 2 * SMOOTH + 2 * step + m - step) * PAD + 8
            return None

        for lon in range(GROUP, LONS - GROUP):
            if lon in EDGE[SENT]:
                j = EDGE[SENT].index(lon)
                source, at, entering = edge_local, SENT * GROUP + j, entering_of(edge_states, slot(EDGE, SENT, j) * STATES)
            else:
                at = lon - INNER[0][0]
                source, entering = local, entering_of(states, at * STATES)
            block = corrected_block(
                lambda level, half: source[slab * SLAB + level, at, 8 * half : 8 * half + 8, :],
                lambda n, level: row(profile_rows, (n * LEVELS + slab * SLAB + level) * LONS + lon),
                entering,
            )
            buffers[0, lon, 8 : 8 + LATS, :] = jnp.transpose(block)

        def edges(to_low, to_high):
            for index, sent in enumerate((to_low, to_high)):
                for j in range(GROUP):
                    lon = EDGE[index][j]
                    block = sent[pl.ds(pl.multiple_of((j * SLABS + slab) * LATS, 8), LATS), :]
                    buffers[0, lon, 8 : 8 + LATS, :] = block
                    start = keep(0, lon)
                    if start is not None:
                        kept_rows[pl.ds(pl.multiple_of(start, 8), LATS), :] = block

        by_core(edges, to_mate, to_other)
        for step in range(SMOOTH):

            def at(which, lon, offset):
                return (which * LONS + lon) * PAD + 8 + offset

            def tile(t, carry):
                source, target = step % 2, (step + 1) % 2
                top = pl.multiple_of(8 * t, 8)
                west = rows[pl.ds(at(source, step, top), 8), :]
                here = rows[pl.ds(at(source, step + 1, top), 8), :]
                for lon in range(step + 1, LONS - step - 1):
                    east = rows[pl.ds(at(source, lon + 1, top), 8), :]
                    north = rows[pl.ds(at(source, lon, top - 1), 8), :]
                    south = rows[pl.ds(at(source, lon, top + 1), 8), :]
                    k = spread_rows[lon, pl.ds(top, 8), :]
                    value = stepped(here, (east + west) + (north + south), k)
                    rows[pl.ds(at(target, lon, top), 8), :] = value
                    start = keep(step + 1, lon)
                    if start is not None:
                        kept_rows[pl.ds(pl.multiple_of(start + top, 8), 8), :] = value
                    west, here = here, east
                return carry

            lax.fori_loop(0, LATS // 8, tile, 0, unroll=4)
        for lon in range(GROUP, LONS - GROUP):
            block = jnp.transpose(buffers[0, lon, 8 : 8 + LATS, :])
            for part in range(2 * SLAB):
                first = slab * SLAB * MEMBERS + 8 * part
                piece = block[8 * part : 8 * part + 8, :]
                if 8 <= lon < 16:
                    made_rows[pl.ds(first * 8 + lon - 8, 8, stride=8), :] = piece
                else:
                    side = lon // 16
                    begun_rows[pl.ds((side * LEVELS * MEMBERS + first) * 8 + lon - 16 * side, 8, stride=8), :] = piece
        save(slab).start()
        return carry

    lax.fori_loop(0, SLABS, run, 0)
    wait_all([save(slab) for slab in range(SLABS)])


def inner_call(local, edge_local, profiles, diffusivity, to_mate, to_other, pieces, edge_pieces):
    return pl.pallas_call(
        inner_kernel,
        out_shape=[
            shape(LEVELS * MEMBERS, LONS, LATS),
            resident(2, LEVELS * MEMBERS, 8, LATS),
            resident(SLABS, 2, 2 * SMOOTH, PAD, LATS),
            resident(LONS, LATS, LATS),
        ],
        in_specs=[ON_CHIP] * 14,
        out_specs=[OFF_CHIP, ON_CHIP, ON_CHIP, ON_CHIP],
        scratch_shapes=[
            pltpu.VMEM((GROUP * len(INNER) * STATES, LATS), F32),
            pltpu.VMEM((GROUP * len(EDGE) * STATES, LATS), F32),
            pltpu.VMEM((2, LONS, PAD, LATS), F32),
            pltpu.VMEM((LEVELS * MEMBERS, 8, LATS), F32),
            pltpu.SemaphoreType.DMA((SLABS,)),
        ],
        compiler_params=ROOM,
        cost_estimate=cost(2 * 10**8),
        name="inner",
    )(local, edge_local, profiles, diffusivity, to_mate, to_other, *pieces, *edge_pieces)


def outer_kernel(whole, begun, kept, spread_rows, mate, other, out, filled, buffers, halo_spread, sems):
    places = 2 * SMOOTH

    def saves(slab):
        part = pl.ds(slab * SLAB * MEMBERS, SLAB * MEMBERS)
        return [
            pltpu.make_async_copy(filled.at[side, part], out.at[part, pl.ds(lon, 8), :], sems.at[slab, side])
            for side, lon in enumerate((0, 16))
        ]

    rows = buffers.reshape(2 * 2 * places * PAD, LATS)
    kept_rows = kept.reshape(SLABS * 2 * 2 * SMOOTH * PAD, LATS)
    clear_pads(rows, 2 * 2 * places)

    def spreads(low, high):
        for side, halo in enumerate((low, high)):
            for j in range(GROUP):
                place = j if side == 0 else GROUP - 1 - j
                at = HALO + (GROUP + j if side == 0 else j)
                halo_spread[side, place] = spread(halo[at : at + 1, :])

    by_core(spreads, mate, other)
    filled_rows = filled.reshape(2 * LEVELS * MEMBERS * 8, LATS)

    def run(slab, carry):
        def halos(low, high):
            for side, halo in enumerate((low, high)):
                for j in range(GROUP):
                    place = j if side == 0 else GROUP - 1 - j
                    block = halo[pl.ds(pl.multiple_of((j * SLABS + slab) * LATS, 8), LATS), :]
                    buffers[0, side, place, 8 : 8 + LATS, :] = block

        by_core(halos, mate, other)
        for step in range(SMOOTH):

            def tile(t, carry):
                top = pl.multiple_of(8 * t, 8)
                for side in range(2):

                    def value_at(place, offset):
                        if place < step + SMOOTH:
                            start = ((step % 2 * 2 + side) * places + place) * PAD
                            return rows[pl.ds(start + 8 + top + offset, 8), :]
                        start = ((slab * 2 + side) * 2 * SMOOTH + 2 * step + place - step - SMOOTH) * PAD
                        return kept_rows[pl.ds(start + 8 + top + offset, 8), :]

                    west, here = value_at(step, 0), value_at(step + 1, 0)
                    for place in range(step + 1, step + SMOOTH + 1):
                        east = value_at(place + 1, 0)
                        around = (east + west) + (value_at(place, -1) + value_at(place, 1))
                        if place < GROUP:
                            k = halo_spread[side, place, pl.ds(top, 8), :]
                        else:
                            m = place - GROUP
                            k = spread_rows[m if side == 0 else LONS - 1 - m, pl.ds(top, 8), :]
                        start = (((step + 1) % 2 * 2 + side) * places + place) * PAD
                        rows[pl.ds(pl.multiple_of(start + 8 + top, 8), 8), :] = stepped(here, around, k)
                        west, here = here, east
                return carry

            lax.fori_loop(0, LATS // 8, tile, 0, unroll=4)
        for side in range(2):
            for m in range(GROUP):
                block = jnp.transpose(buffers[0, side, GROUP + m, 8 : 8 + LATS, :])
                for part in range(2 * SLAB):
                    first = (side * LEVELS + slab * SLAB) * MEMBERS + 8 * part
                    lon = m if side == 0 else 7 - m
                    filled_rows[pl.ds(first * 8 + lon, 8, stride=8), :] = block[8 * part : 8 * part + 8, :]
        start_all(saves(slab))
        return carry

    lax.fori_loop(0, SLABS, run, 0)
    for slab in range(SLABS):
        wait_all(saves(slab))


def outer_call(whole, begun, kept, spread_rows, mate, other):
    return pl.pallas_call(
        outer_kernel,
        out_shape=[shape(LEVELS * MEMBERS, LONS, LATS), resident(2, LEVELS * MEMBERS, 8, LATS)],
        in_specs=[OFF_CHIP] + [ON_CHIP] * 5,
        out_specs=[OFF_CHIP, ON_CHIP],
        input_output_aliases={0: 0, 1: 1},
        scratch_shapes=[
            pltpu.VMEM((2, 2, 2 * SMOOTH, PAD, LATS), F32),
            pltpu.VMEM((2, GROUP, LATS, LATS), F32),
            pltpu.SemaphoreType.DMA((SLABS, 2)),
        ],
        compiler_params=ROOM,
        name="outer",
    )(whole, begun, kept, spread_rows, mate, other)


def shifted(pieces):
    moved = [pieces[0]]
    for at in (1, 2, 3):
        moved.append(lax.ppermute(pieces[at], "lev", [(i, i ^ PARTNERS[at]) for i in range(BLOCKS)]))
    return moved


def exchanged(to_mate, to_other):
    count = lax.axis_size("col")
    both_ways = lambda first: [pair for i in range(first, count - 1, 2) for pair in ((i, i + 1), (i + 1, i))]
    other = lax.ppermute(to_other, "col", both_ways(1))
    mate = lax.ppermute(to_mate, "col", both_ways(0))
    return mate, other


def per_device(control_field, decay_rate, diffusivity):
    field = control_field.reshape(LEVELS * MEMBERS, LONS, LATS)
    edge_local, *edge_pieces, profiles, table, xs, rates = edge_sweep_call(field, decay_rate)
    inner_local, *inner_pieces = inner_sweep_call(xs, rates, table)
    edge_states = shifted(solve_call(shifted(edge_pieces)))
    inner_states = shifted(solve_call(shifted(inner_pieces)))
    to_mate, to_other = edge_call(edge_local, profiles, diffusivity, edge_states)
    mate, other = exchanged(to_mate, to_other)
    whole, begun, kept, spread_rows = inner_call(inner_local, edge_local, profiles, diffusivity, to_mate, to_other, inner_states, edge_states)
    out, _ = outer_call(whole, begun, kept, spread_rows, mate, other)
    return out.reshape(control_field.shape)


def solution(mesh):
    in_specs = (P("lev", None, "col", None), P("lev", "col", None), P("col", None))
    out_specs = P("lev", None, "col", None)
    return jax.shard_map(
        per_device, mesh=mesh, in_specs=in_specs, out_specs=out_specs, check_vma=False
    )
```

```python
import functools

import jax
import jax.numpy as jnp
from jax import lax
from jax.experimental import pallas as pl
from jax.experimental.pallas import tpu as pltpu
from jax.sharding import PartitionSpec as P


SMOOTH = 4
LEVELS = 24
MEMBERS = 16
LONS = 24
LATS = 128
BLOCKS = 4
PARTNERS = (0, 3, 2, 1)
RECORD = 72
STATES = 64
GROUP = 4
EDGE = ((0, 1, 2, 3), (20, 21, 22, 23), (4, 5, 18, 19))
INNER = ((6, 7, 8, 9), (10, 11, 12, 13), (14, 15, 16, 17))
SENT = 2
SLAB = 8
SLABS = LEVELS // SLAB
PAD = LATS + 24
HALO = GROUP * SLABS * LATS

OFF_CHIP = pl.BlockSpec(memory_space=pltpu.HBM)
ON_CHIP = pl.BlockSpec(memory_space=pltpu.VMEM)
ROOM = pltpu.CompilerParams(vmem_limit_bytes=28 * 2**20)
F32 = jnp.float32


def cost(flops):
    return pl.CostEstimate(flops=flops, transcendentals=0, bytes_accessed=10**6)


def shape(*dims):
    return jax.ShapeDtypeStruct(dims, F32)


def resident(*dims):
    return pltpu.VMEM(dims, F32)


def row(ref, at):
    return ref[pl.ds(at, 8, stride=0), :]


def slot(groups, index, j):
    return len(groups) * j + index if groups == EDGE else GROUP * index + j


def in_order(pieces, target, rows):
    here = lax.axis_index("lev")
    for mask, piece in zip(PARTNERS, pieces):
        source = jnp.bitwise_xor(here, mask)
        target[pl.ds(pl.multiple_of(source * rows, 8), rows), :] = piece[...]


def responses(rates, profiles, scratch):
    tiles = [slice(8 * tile, 8 * tile + 8) for tile in range(LONS // 8)]
    up, down = range(LEVELS), range(LEVELS - 1, -1, -1)

    def sweep(order, source, target):
        state = [None] * len(tiles)
        for level in order:
            for at, lons in enumerate(tiles):
                rate = rates[level, lons, :]
                if source is None:
                    state[at] = rate if state[at] is None else rate * state[at]
                else:
                    value = (1.0 - rate) * source[level, lons, :]
                    state[at] = value if state[at] is None else rate * state[at] + value
                target[level, lons, :] = state[at]
        return state

    through = sweep(up, None, scratch.at[0])
    sweep(down, None, profiles.at[3])
    q21 = sweep(down, scratch.at[0], profiles.at[2])
    q32 = sweep(up, profiles.at[3], scratch.at[1])
    q31 = sweep(up, profiles.at[2], scratch.at[0])
    q42 = sweep(down, scratch.at[1], profiles.at[1])
    q41 = sweep(down, scratch.at[0], profiles.at[0])
    return through, q21, q31, q32, q41, q42


def sweep_groups(groups, xs, rates, table, local, exits, before):
    values = xs.reshape(LEVELS * MEMBERS * LONS, LATS)
    weights = rates.reshape(LEVELS * LONS, LATS)

    def run(index, carry):
        lons = groups[index] if isinstance(index, int) else [groups[0][0] + GROUP * index + j for j in range(GROUP)]
        for number in range(4):
            order = range(LEVELS) if number % 2 == 0 else range(LEVELS - 1, -1, -1)
            state = {}
            for level in order:
                for j in range(GROUP):
                    weight = row(weights, level * LONS + lons[j])
                    rest = 1.0 - weight
                    for half in range(2):
                        if number == 0:
                            start = (level * MEMBERS + 8 * half) * LONS + lons[j]
                            value = values[pl.ds(start, 8, stride=LONS), :]
                        else:
                            value = local[level, GROUP * index + j, 8 * half : 8 * half + 8, :]
                        value = rest * value
                        if (j, half) in state:
                            value = weight * state[j, half] + value
                        state[j, half] = value
                        local[level, GROUP * index + j, 8 * half : 8 * half + 8, :] = value
            for (j, half), value in state.items():
                place = slot(groups, index, j) * RECORD + 16 * number + 8 * half
                exits[pl.ds(place if isinstance(place, int) else pl.multiple_of(place, 8), 8), :] = value
        return carry

    for index, group in enumerate(groups):
        for j in range(GROUP):
            lon = group[j]
            for which in range(6):
                record = slot(groups, index, j) * RECORD + STATES + which
                exits[record : record + 1, :] = table[which, lon : lon + 1, :]
    if groups == EDGE:
        for index in range(len(groups)):
            before[index]()
            run(index, 0)
    else:
        lax.fori_loop(0, len(groups), run, 0)


def share_out(exits, pieces, rows):
    here = lax.axis_index("lev")
    for mask, piece in zip(PARTNERS, pieces):
        target = jnp.bitwise_xor(here, mask)
        piece[...] = exits[pl.ds(pl.multiple_of(target * rows, 8), rows), :]


def edge_sweep_kernel(field, rate, local, p0, p1, p2, p3, profiles, table, xs, rates, exits, scratch, sems):
    small = pltpu.make_async_copy(rate, rates, sems.at[3])
    small.start()
    loads = {}
    for tile in (0, 2, 1):
        lons = pl.ds(8 * tile, 8)
        loads[tile] = pltpu.make_async_copy(field.at[:, lons, :], xs.at[:, lons, :], sems.at[tile])
        loads[tile].start()
    small.wait()
    for which, tiles in enumerate(responses(rates, profiles, scratch)):
        for tile, value in enumerate(tiles):
            table[which, 8 * tile : 8 * tile + 8, :] = value
    sweep_groups(EDGE, xs, rates, table, local, exits, [loads[0].wait, loads[2].wait, lambda: None])
    share_out(exits, (p0, p1, p2, p3), len(EDGE) * RECORD)
    loads[1].wait()


def edge_sweep_call(field, rate):
    count = GROUP * len(EDGE)
    outs = [resident(LEVELS, count, MEMBERS, LATS)] + [resident(len(EDGE) * RECORD, LATS)] * BLOCKS
    outs += [resident(4, LEVELS, LONS, LATS), resident(6, LONS, LATS), resident(LEVELS * MEMBERS, LONS, LATS), resident(LEVELS, LONS, LATS)]
    return pl.pallas_call(
        edge_sweep_kernel,
        out_shape=outs,
        in_specs=[OFF_CHIP] * 2,
        out_specs=[ON_CHIP] * len(outs),
        scratch_shapes=[
            pltpu.VMEM((count * RECORD, LATS), F32),
            pltpu.VMEM((2, LEVELS, LONS, LATS), F32),
            pltpu.SemaphoreType.DMA((4,)),
        ],
        compiler_params=ROOM,
        cost_estimate=cost(3 * 10**7),
        name="edge_sweeps",
    )(*(pltpu.with_memory_space_constraint(x, pltpu.HBM) for x in (field, rate)))


def inner_sweep_kernel(xs, rates, table, local, p0, p1, p2, p3, exits):
    sweep_groups(INNER, xs, rates, table, local, exits, None)
    share_out(exits, (p0, p1, p2, p3), len(INNER) * RECORD)


def inner_sweep_call(xs, rates, table):
    count = GROUP * len(INNER)
    outs = [resident(LEVELS, count, MEMBERS, LATS)] + [resident(len(INNER) * RECORD, LATS)] * BLOCKS
    return pl.pallas_call(
        inner_sweep_kernel,
        out_shape=outs,
        in_specs=[ON_CHIP] * 3,
        out_specs=[ON_CHIP] * len(outs),
        scratch_shapes=[pltpu.VMEM((count * RECORD, LATS), F32)],
        compiler_params=ROOM,
        cost_estimate=cost(5 * 10**7),
        name="inner_sweeps",
    )(xs, rates, table)


def solve_kernel(share, *refs):
    pieces, outs, (records, states) = refs[:4], refs[4:8], refs[8:]
    in_order(pieces, records, share * RECORD)

    def run(lon, carry):
        def exit_of(block, number, half):
            at = (block * share + lon) * RECORD + 16 * number + 8 * half
            return records[pl.ds(pl.multiple_of(at, 8), 8), :]

        def response(block, which):
            return row(records, (block * share + lon) * RECORD + STATES + which)

        for half in range(2):
            zero = jnp.zeros((8, LATS), F32)
            f1, b1, f2, b2 = ([zero] * BLOCKS for _ in range(4))
            for d in range(BLOCKS - 1):
                f1[d + 1] = exit_of(d, 0, half) + response(d, 0) * f1[d]
            for d in range(BLOCKS - 1, 0, -1):
                b1[d - 1] = exit_of(d, 1, half) + response(d, 1) * f1[d] + response(d, 0) * b1[d]
            for d in range(BLOCKS - 1):
                f2[d + 1] = (
                    exit_of(d, 2, half)
                    + response(d, 2) * f1[d]
                    + response(d, 3) * b1[d]
                    + response(d, 0) * f2[d]
                )
            for d in range(BLOCKS - 1, 0, -1):
                b2[d - 1] = (
                    exit_of(d, 3, half)
                    + response(d, 4) * f1[d]
                    + response(d, 5) * b1[d]
                    + response(d, 1) * f2[d]
                    + response(d, 0) * b2[d]
                )
            for d in range(BLOCKS):
                for number, entering in enumerate((f1, b1, f2, b2)):
                    at = (d * share + lon) * STATES + 16 * number + 8 * half
                    states[pl.ds(pl.multiple_of(at, 8), 8), :] = entering[d]
        return carry

    lax.fori_loop(0, share, run, 0)
    share_out(states, outs, share * STATES)


def solve_call(pieces):
    share = pieces[0].shape[0] // RECORD
    return pl.pallas_call(
        functools.partial(solve_kernel, share),
        out_shape=[resident(share * STATES, LATS)] * BLOCKS,
        in_specs=[ON_CHIP] * BLOCKS,
        out_specs=[ON_CHIP] * BLOCKS,
        scratch_shapes=[
            pltpu.VMEM((BLOCKS * share * RECORD, LATS), F32),
            pltpu.VMEM((BLOCKS * share * STATES, LATS), F32),
        ],
        compiler_params=ROOM,
    )(*pieces)


def corrected_block(value_of, profile_of, entering):
    parts = []
    for level in range(SLAB):
        mine = [profile_of(n, level) for n in range(4)]
        for half in range(2):
            value = value_of(level, half)
            for n in range(4):
                value = value + mine[n] * entering[half][n]
            parts.append(value)
    return jnp.concatenate(parts, axis=0)


def entering_of(states, start):
    return [[states[pl.ds(start + 16 * n + 8 * half, 8), :] for n in range(4)] for half in range(2)]


def spread(kappa, lon):
    return jnp.transpose(jnp.concatenate([row(kappa, lon)] * (LATS // 8), axis=0))


def by_core(act, mate, other):
    odd = lax.rem(lax.axis_index("col"), 2)
    pl.when(odd == 0)(lambda: act(other, mate))
    pl.when(odd == 1)(lambda: act(mate, other))


def stepped(here, around, k):
    return here + k * (around - 4.0 * here)


def clear_pads(rows, blocks):
    zero = jnp.zeros((8, LATS), F32)
    for block in range(blocks):
        rows[block * PAD : block * PAD + 8, :] = zero
        rows[block * PAD + LATS + 8 : block * PAD + LATS + 16, :] = zero


def edge_kernel(local, profiles, kappa, s0, s1, s2, s3, to_mate, to_other, states):
    odd = lax.rem(lax.axis_index("col"), 2)
    in_order((s0, s1, s2, s3), states, len(EDGE) * STATES)
    profile_rows = profiles.reshape(4 * LEVELS * LONS, LATS)
    sides = ((to_mate, 1 - odd), (to_other, odd))
    for out, index in sides:
        out[HALO : HALO + 8, :] = kappa[pl.ds(pl.multiple_of(16 * index, 8), 8), :]

    def run(slab, carry):
        for out, index in sides:
            for j in range(GROUP):
                lon = (LONS - GROUP) * index + j
                block = corrected_block(
                    lambda level, half: local[slab * SLAB + level, GROUP * index + j, 8 * half : 8 * half + 8, :],
                    lambda n, level: row(profile_rows, (n * LEVELS + slab * SLAB + level) * LONS + lon),
                    entering_of(states, pl.multiple_of(slot(EDGE, index, j) * STATES, 8)),
                )
                out[pl.ds(pl.multiple_of((j * SLABS + slab) * LATS, 8), LATS), :] = jnp.transpose(block)
        return carry

    lax.fori_loop(0, SLABS, run, 0)


def edge_call(local, profiles, diffusivity, pieces):
    return pl.pallas_call(
        edge_kernel,
        out_shape=[resident(HALO + 8, LATS)] * 2,
        in_specs=[ON_CHIP] * 7,
        out_specs=[ON_CHIP] * 2,
        scratch_shapes=[pltpu.VMEM((GROUP * len(EDGE) * STATES, LATS), F32)],
        compiler_params=ROOM,
        cost_estimate=cost(10**7),
        name="edges",
    )(local, profiles, diffusivity, *pieces)


def inner_kernel(local, edge_local, profiles, spread_rows, to_mate, to_other, *refs):
    pieces, edge_pieces, refs = refs[:4], refs[4:8], refs[8:]
    made, begun, kept, states, edge_states, buffers = refs

    in_order(pieces, states, len(INNER) * STATES)
    in_order(edge_pieces, edge_states, len(EDGE) * STATES)
    rows = buffers.reshape(2 * LONS * PAD, LATS)
    kept_rows = kept.reshape(SLABS * 2 * 2 * SMOOTH * PAD, LATS)
    clear_pads(rows, 2 * LONS)
    clear_pads(kept_rows, SLABS * 2 * 2 * SMOOTH)
    profile_rows = profiles.reshape(4 * LEVELS * LONS, LATS)
    made_rows = made.reshape(LEVELS * MEMBERS * 8, LATS)
    begun_rows = begun.reshape(2 * LEVELS * MEMBERS * 8, LATS)

    def run(slab, carry):
        def keep(step, lon):
            for side, m in enumerate((lon, LONS - 1 - lon)):
                if step <= m < step + 2 and step < SMOOTH:
                    return ((slab * 2 + side) * 2 * SMOOTH + 2 * step + m - step) * PAD + 8
            return None

        for lon in range(GROUP, LONS - GROUP):
            if lon in EDGE[SENT]:
                j = EDGE[SENT].index(lon)
                source, at, entering = edge_local, SENT * GROUP + j, entering_of(edge_states, slot(EDGE, SENT, j) * STATES)
            else:
                at = lon - INNER[0][0]
                source, entering = local, entering_of(states, at * STATES)
            block = corrected_block(
                lambda level, half: source[slab * SLAB + level, at, 8 * half : 8 * half + 8, :],
                lambda n, level: row(profile_rows, (n * LEVELS + slab * SLAB + level) * LONS + lon),
                entering,
            )
            buffers[0, lon, 8 : 8 + LATS, :] = jnp.transpose(block)

        def edges(to_low, to_high):
            for index, sent in enumerate((to_low, to_high)):
                for j in range(GROUP):
                    lon = EDGE[index][j]
                    block = sent[pl.ds(pl.multiple_of((j * SLABS + slab) * LATS, 8), LATS), :]
                    buffers[0, lon, 8 : 8 + LATS, :] = block
                    start = keep(0, lon)
                    if start is not None:
                        kept_rows[pl.ds(pl.multiple_of(start, 8), LATS), :] = block

        by_core(edges, to_mate, to_other)
        for step in range(SMOOTH):

            def at(which, lon, offset):
                return (which * LONS + lon) * PAD + 8 + offset

            def tile(t, carry):
                source, target = step % 2, (step + 1) % 2
                top = pl.multiple_of(8 * t, 8)
                west = rows[pl.ds(at(source, step, top), 8), :]
                here = rows[pl.ds(at(source, step + 1, top), 8), :]
                for lon in range(step + 1, LONS - step - 1):
                    east = rows[pl.ds(at(source, lon + 1, top), 8), :]
                    north = rows[pl.ds(at(source, lon, top - 1), 8), :]
                    south = rows[pl.ds(at(source, lon, top + 1), 8), :]
                    k = spread_rows[lon, pl.ds(top, 8), :]
                    value = stepped(here, (east + west) + (north + south), k)
                    rows[pl.ds(at(target, lon, top), 8), :] = value
                    start = keep(step + 1, lon)
                    if start is not None:
                        kept_rows[pl.ds(pl.multiple_of(start + top, 8), 8), :] = value
                    west, here = here, east
                return carry

            lax.fori_loop(0, LATS // 8, tile, 0, unroll=8)
        for lon in range(GROUP, LONS - GROUP):
            block = jnp.transpose(buffers[0, lon, 8 : 8 + LATS, :])
            for part in range(2 * SLAB):
                first = slab * SLAB * MEMBERS + 8 * part
                piece = block[8 * part : 8 * part + 8, :]
                if 8 <= lon < 16:
                    made_rows[pl.ds(first * 8 + lon - 8, 8, stride=8), :] = piece
                else:
                    side = lon // 16
                    begun_rows[pl.ds((side * LEVELS * MEMBERS + first) * 8 + lon - 16 * side, 8, stride=8), :] = piece
        return carry

    lax.fori_loop(0, SLABS, run, 0)


def spread_kernel(kappa, spread_rows):
    for lon in range(LONS):
        spread_rows[lon] = spread(kappa, lon)


def spread_call(diffusivity):
    return pl.pallas_call(
        spread_kernel,
        out_shape=resident(LONS, LATS, LATS),
        in_specs=[ON_CHIP],
        out_specs=ON_CHIP,
        compiler_params=ROOM,
        name="spreads",
    )(diffusivity)


def inner_call(local, edge_local, profiles, spread_rows, to_mate, to_other, pieces, edge_pieces):
    return pl.pallas_call(
        inner_kernel,
        out_shape=[
            resident(LEVELS * MEMBERS, 8, LATS),
            resident(2, LEVELS * MEMBERS, 8, LATS),
            resident(SLABS, 2, 2 * SMOOTH, PAD, LATS),
        ],
        in_specs=[ON_CHIP] * 14,
        out_specs=[ON_CHIP] * 3,
        scratch_shapes=[
            pltpu.VMEM((GROUP * len(INNER) * STATES, LATS), F32),
            pltpu.VMEM((GROUP * len(EDGE) * STATES, LATS), F32),
            pltpu.VMEM((2, LONS, PAD, LATS), F32),
        ],
        compiler_params=ROOM,
        cost_estimate=cost(2 * 10**8),
        name="inner",
    )(local, edge_local, profiles, spread_rows, to_mate, to_other, *pieces, *edge_pieces)


def outer_kernel(of_mate, *refs):
    if of_mate:
        whole, begun, kept, spread_rows, halo, out, filled, buffers, halo_spread, sems = refs
    else:
        _, begun, kept, spread_rows, halo, out, filled, buffers, halo_spread, sems = refs
    odd = lax.rem(lax.axis_index("col"), 2)
    side = 1 - odd if of_mate else odd
    places = 2 * SMOOTH

    def saves(slab):
        part = pl.ds(slab * SLAB * MEMBERS, SLAB * MEMBERS)
        tile = pl.ds(pl.multiple_of(16 * side, 8), 8)
        return pltpu.make_async_copy(filled.at[side, part], out.at[part, tile, :], sems.at[slab])

    if of_mate:
        middle = pltpu.make_async_copy(whole, out.at[:, pl.ds(8, 8), :], sems.at[SLABS])
        middle.start()
    rows = buffers.reshape(2 * places * PAD, LATS)
    kept_rows = kept.reshape(SLABS * 2 * 2 * SMOOTH * PAD, LATS)
    filled_rows = filled.reshape(2 * LEVELS * MEMBERS * 8, LATS)
    clear_pads(rows, 2 * places)
    for place in range(GROUP):
        j = jnp.where(side == 0, place, GROUP - 1 - place)
        halo_spread[place] = spread(halo, HALO + j + GROUP * (1 - side))

    def run(slab, carry):
        for place in range(GROUP):
            j = jnp.where(side == 0, place, GROUP - 1 - place)
            buffers[0, place, 8 : 8 + LATS, :] = halo[pl.ds(pl.multiple_of((j * SLABS + slab) * LATS, 8), LATS), :]
        for step in range(SMOOTH):

            def tile(t, carry):
                top = pl.multiple_of(8 * t, 8)

                def value_at(place, offset):
                    if place < step + SMOOTH:
                        return rows[pl.ds((step % 2 * places + place) * PAD + 8 + top + offset, 8), :]
                    start = ((slab * 2 + side) * 2 * SMOOTH + 2 * step + place - step - SMOOTH) * PAD
                    return kept_rows[pl.ds(start + 8 + top + offset, 8), :]

                west, here = value_at(step, 0), value_at(step + 1, 0)
                for place in range(step + 1, step + SMOOTH + 1):
                    east = value_at(place + 1, 0)
                    around = (east + west) + (value_at(place, -1) + value_at(place, 1))
                    if place < GROUP:
                        k = halo_spread[place, pl.ds(top, 8), :]
                    else:
                        m = place - GROUP
                        k = spread_rows[jnp.where(side == 0, m, LONS - 1 - m), pl.ds(top, 8), :]
                    start = ((step + 1) % 2 * places + place) * PAD
                    rows[pl.ds(pl.multiple_of(start + 8 + top, 8), 8), :] = stepped(here, around, k)
                    west, here = here, east
                return carry

            lax.fori_loop(0, LATS // 8, tile, 0, unroll=16)
        for m in range(GROUP):
            block = jnp.transpose(buffers[0, GROUP + m, 8 : 8 + LATS, :])
            lon = jnp.where(side == 0, m, 7 - m)
            for part in range(2 * SLAB):
                first = (side * LEVELS + slab * SLAB) * MEMBERS + 8 * part
                filled_rows[pl.ds(first * 8 + lon, 8, stride=8), :] = block[8 * part : 8 * part + 8, :]
        saves(slab).start()
        return carry

    lax.fori_loop(0, SLABS, run, 0)
    if of_mate:
        middle.wait()
    for slab in range(SLABS):
        saves(slab).wait()


def outer_call(of_mate, whole, begun, kept, spread_rows, halo):
    return pl.pallas_call(
        functools.partial(outer_kernel, of_mate),
        out_shape=[shape(LEVELS * MEMBERS, LONS, LATS), resident(2, LEVELS * MEMBERS, 8, LATS)],
        in_specs=[ON_CHIP if of_mate else OFF_CHIP] + [ON_CHIP] * 4,
        out_specs=[OFF_CHIP, ON_CHIP],
        input_output_aliases={1: 1} if of_mate else {0: 0, 1: 1},
        scratch_shapes=[
            pltpu.VMEM((2, 2 * SMOOTH, PAD, LATS), F32),
            pltpu.VMEM((GROUP, LATS, LATS), F32),
            pltpu.SemaphoreType.DMA((SLABS + 1,)),
        ],
        compiler_params=ROOM,
        cost_estimate=cost(4 * 10**7),
        name="outer_mate" if of_mate else "outer_other",
    )(whole, begun, kept, spread_rows, halo)


def shifted(pieces):
    moved = [pieces[0]]
    for at in (1, 2, 3):
        moved.append(lax.ppermute(pieces[at], "lev", [(i, i ^ PARTNERS[at]) for i in range(BLOCKS)]))
    return moved


def exchanged(to_mate, to_other):
    count = lax.axis_size("col")
    both_ways = lambda first: [pair for i in range(first, count - 1, 2) for pair in ((i, i + 1), (i + 1, i))]
    other = lax.ppermute(to_other, "col", both_ways(1))
    mate = lax.ppermute(to_mate, "col", both_ways(0))
    return mate, other


def per_device(control_field, decay_rate, diffusivity):
    field = control_field.reshape(LEVELS * MEMBERS, LONS, LATS)
    edge_local, *edge_pieces, profiles, table, xs, rates = edge_sweep_call(field, decay_rate)
    inner_local, *inner_pieces = inner_sweep_call(xs, rates, table)
    edge_states = shifted(solve_call(shifted(edge_pieces)))
    inner_states = shifted(solve_call(shifted(inner_pieces)))
    to_mate, to_other = edge_call(edge_local, profiles, diffusivity, edge_states)
    mate, other = exchanged(to_mate, to_other)
    spread_rows = spread_call(diffusivity)
    made, begun, kept = inner_call(inner_local, edge_local, profiles, spread_rows, to_mate, to_other, inner_states, edge_states)
    whole, begun = outer_call(True, made, begun, kept, spread_rows, mate)
    out, _ = outer_call(False, whole, begun, kept, spread_rows, other)
    return out.reshape(control_field.shape)


def solution(mesh):
    in_specs = (P("lev", None, "col", None), P("lev", "col", None), P("col", None))
    out_specs = P("lev", None, "col", None)
    return jax.shard_map(
        per_device, mesh=mesh, in_specs=in_specs, out_specs=out_specs, check_vma=False
    )
```
